32 devices in a mesh: pop: 8 (over y, x, core), tile: 4 (over z).
Axes of the slice: x: 2, y: 2, z: 4, core: 2. Of those that a mesh axis runs over, the one named last changes fastest.
Arguments:
- weights: int32 [8, 8], replicated, may hold values from -2 to 3
- terminal: float32 [8, 32, 2048], P('pop', 'tile'), may hold values from -4.5 to 4.5
- density_history: bfloat16 [8, 8, 32, 2048], P('pop', None, 'tile'), may hold values from 0.19921875 to 2
- density_init: float32 [8, 32, 2048], P('pop', 'tile'), may hold values from 0.2 to 2
Outputs:
- values: float32 [8, 8, 32, 2048], P('pop', None, 'tile')
- density_final: float32 [8, 32, 2048], P('pop', 'tile')
The draws below stay inside these ranges and needn't reach their ends.
All inputs are finite; a program needn't handle non-finite values.
Results may differ from the reference program's by a relative error of at most 0.0003.
Values may be sent and summed in bfloat16 or wider, within the bound.
A program may use at most 64 MiB of HBM per device.

```python
import math
import jax
import jax.numpy as jnp
from jax import lax

COLS = 2048
STEPS = 8
POPS = 8
ROWS = 32


def draw_terminal(key, part):
    slope_key = jax.random.fold_in(key, 11)
    phase_key = jax.random.fold_in(key, 12)
    noise_key = jax.random.fold_in(key, 13)
    period = 12.0
    phase = jax.random.randint(phase_key, (POPS, 1, 1), 0, 12).astype(jnp.float32)
    rows = jnp.arange(ROWS, dtype=jnp.float32)[None, :, None]
    position = jnp.mod(rows + phase, period)
    ramp = jnp.abs(position - 0.5 * period) - 0.25 * period
    slope = jax.random.uniform(slope_key, (POPS, 1, 1), jnp.float32, 1.0, 1.25)
    noise = 0.2 * jnp.clip(jax.random.normal(noise_key, (POPS, ROWS, COLS), jnp.float32), -3.0, 3.0)
    return slope * ramp + noise


def set_ends(values, own_key, least, largest):
    extent = values.shape
    place = [jax.random.randint(jax.random.fold_in(own_key, axis), (), 0, extent[axis]) for axis in range(len(extent))]
    values = values.at[tuple(place)].set(least)
    longest = extent.index(max(extent))
    place[longest] = (place[longest] + 1) % extent[longest]
    return values.at[tuple(place)].set(largest)


def level_of(key, shape, cuts, least, high):
    loudness = 1.0
    for dim, parts in cuts:
        draws = jax.random.uniform(jax.random.fold_in(jax.random.fold_in(key, 6), dim), (parts,), jnp.float32, least / len(cuts), high / len(cuts))
        loudness = loudness * jnp.repeat(jnp.exp(draws), shape[dim] // parts).reshape((-1,) + (1,) * (len(shape) - 1 - dim))
    return loudness


def setup_inputs(seed: int = 0) -> dict:
    keys = jax.random.split(jax.random.key(seed), 5)
    weights = set_ends(jax.random.randint(keys[0], (POPS, POPS), -2, 4), jax.random.fold_in(keys[0], 1), -2, 3).astype(jnp.int32)
    terminal = draw_terminal(jax.random.fold_in(keys[4], 71), 0)
    density_history = jnp.clip(jnp.exp(math.log(2.0) - 2.306499 * jax.random.uniform(keys[2], (POPS, STEPS, ROWS, COLS), jnp.float32) ** level_of(keys[2], (POPS, STEPS, ROWS, COLS), ((0, 8), (2, 4)), -0.2, 0.2)), 0.19921875, 2.0).astype(jnp.bfloat16)
    density_init = jnp.clip(jnp.exp(math.log(2.0) - 2.3025851 * jax.random.uniform(keys[3], (POPS, ROWS, COLS), jnp.float32) ** level_of(keys[3], (POPS, ROWS, COLS), ((0, 8), (1, 4)), -0.2, 0.2)), 0.2, 2.0)
    return dict(weights=weights, terminal=terminal, density_history=density_history, density_init=density_init)


time_step = 0.2
viscosity = 0.2


def laplace(field):
    return jnp.roll(field, -1, 1) + jnp.roll(field, 1, 1) + jnp.roll(field, -1, 2) + jnp.roll(field, 1, 2) - 4.0 * field


def hamiltonian(field):
    ahead_rows = jnp.minimum(jnp.roll(field, -1, 1) - field, 0.0)
    behind_rows = jnp.maximum(field - jnp.roll(field, 1, 1), 0.0)
    ahead_cols = jnp.minimum(jnp.roll(field, -1, 2) - field, 0.0)
    behind_cols = jnp.maximum(field - jnp.roll(field, 1, 2), 0.0)
    return 0.5 * (behind_rows * behind_rows + ahead_rows * ahead_rows + behind_cols * behind_cols + ahead_cols * ahead_cols)


def transport(density, value):
    drift_rows = -(jnp.roll(value, -1, 1) - value)
    flux_rows = jnp.maximum(drift_rows, 0.0) * density + jnp.minimum(drift_rows, 0.0) * jnp.roll(density, -1, 1)
    drift_cols = -(jnp.roll(value, -1, 2) - value)
    flux_cols = jnp.maximum(drift_cols, 0.0) * density + jnp.minimum(drift_cols, 0.0) * jnp.roll(density, -1, 2)
    div_rows = flux_rows - jnp.roll(flux_rows, 1, 1)
    div_cols = flux_cols - jnp.roll(flux_cols, 1, 2)
    return density + time_step * (viscosity * laplace(density) - div_rows - div_cols)


def reference(weights, terminal, density_history, density_init):
    factors = weights.astype(jnp.float32)
    current = terminal
    centred = [None] * STEPS
    for step in reversed(range(STEPS)):
        coupled = jnp.einsum("pq,qrc->prc", factors, density_history[:, step].astype(jnp.float32), precision=lax.Precision.HIGHEST) / POPS
        advanced = current + time_step * (viscosity * laplace(current) - hamiltonian(current) + coupled)
        advanced = advanced - jnp.mean(advanced, axis=(1, 2), keepdims=True)
        centred[step] = advanced
        current = advanced
    density = density_init
    for step in range(STEPS):
        density = transport(density, centred[step])
    return jnp.stack(centred, axis=1), density
```

```python
import functools

import jax
import jax.numpy as jnp
from jax import lax
from jax.experimental import pallas as pl
from jax.experimental.pallas import tpu as pltpu
from jax.sharding import PartitionSpec as P

time_step = 0.2
viscosity = 0.2
LANES = 128
CHUNK = 512
CENTRE = 1.1
LARGEST = 3.0 * 0.901
LEVELS = 32400.0
RELAY = (2.6, 0.65)
PARTIAL = (3.6, 0.65)
TOTAL = (6.5, 0.65)
SWEEP = (10.3, 0.8)


def kernel(pops, tiles, weights, terminal_in, history_in, initial_in, values, density_out,
           terminal, history, initial, load_sem, near, own_sum, part_out, part_in, cost_out, cost_in,
           value_out, start_value, mass_out, start_mass, swept, mass_main, slope_r, slope_c, sums_own, sums_all,
           near_send, near_recv, part_send, part_recv, cost_send, cost_recv, start_send, start_recv,
           back_send, back_recv, back_self):
    steps, rows, cols = history.shape
    width = cols // tiles
    full = width + LANES
    total_rows = tiles * rows
    outer = pops // 4
    me = lax.axis_index("tile")
    own = lax.axis_index("pop")
    core = own % 2
    plane = (own // 2) % 2
    line = own // 4

    def pop_of(a, b, c):
        return (a * 2 + b) * 2 + c

    partner = pop_of(line, plane, 1 - core)
    across = pop_of(line, 1 - plane, core)
    beyond = pop_of(line, 1 - plane, 1 - core)
    columns = [pop_of((line + j) % outer, plane, core) for j in range(1, outer)]
    peers = [(me + d) % tiles for d in range(1, tiles)]

    barrier = pltpu.get_barrier_semaphore()
    greeted = [{"tile": z} for z in peers] + [{"pop": q} for q in [partner, across] + columns]
    for there in greeted:
        pl.semaphore_signal(barrier, inc=1, device_id=there, device_id_type=pl.DeviceIdType.MESH)

    loads = [pltpu.make_async_copy(src, dst, load_sem.at[n]) for n, (src, dst) in enumerate(
        [(terminal_in, terminal), (initial_in, initial), (history_in, history)])]
    for load in loads:
        load.start()
    for load in loads:
        load.wait()
    right_side = lax.broadcasted_iota(jnp.int32, (rows, LANES), 1) < LANES // 2

    def main_of(block, z):
        return block[:, z * width:(z + 1) * width]

    def rim_of(block, z):
        right = ((z + 1) % tiles) * width
        left = ((z + tiles - 1) % tiles) * width + width - LANES
        return jnp.where(right_side, block[:, right:right + LANES], block[:, left:left + LANES])

    for src, dst in [(terminal, value_out), (initial, mass_out)]:
        block = src[...]
        for z in range(tiles):
            dst[z, :, :width] = main_of(block, z)
            dst[z, :, width:] = rim_of(block, z)
    start_value[me] = value_out[me]
    start_mass[me] = mass_out[me]

    pl.semaphore_wait(barrier, len(greeted))

    def cut(z):
        return pl.ds(pl.multiple_of(z * width, LANES), width)

    sent = []

    def remote(src, dst, send, recv, there):
        copy = pltpu.make_async_remote_copy(src_ref=src, dst_ref=dst, send_sem=send, recv_sem=recv,
                                            device_id=there, device_id_type=pl.DeviceIdType.MESH)
        copy.start()
        return copy

    def arrived(ref, sem):
        pltpu.make_async_copy(ref, ref, sem).wait()

    def spread(src, dst, send, recv):
        for z in peers:
            remote(src.at[z], dst.at[me], send, recv, {"tile": z})

    def wait_spread(dst, sem):
        arrived(dst.at[pl.ds(0, tiles - 1)], sem)

    for n in range(steps):
        t = steps - 1 - n
        sent.append(remote(history.at[t], near.at[1, t], near_send.at[1, n], near_recv.at[1, n], {"pop": across}))
        sent.append(remote(history.at[t], near.at[0, t], near_send.at[0, n], near_recv.at[0, n], {"pop": partner}))
    spread(value_out, start_value, start_send.at[0], start_recv.at[0])
    spread(mass_out, start_mass, start_send.at[1], start_recv.at[1])

    def weight(p, q):
        return weights[p, q].astype(jnp.float32) * (1.0 / pops)

    sources = [own, partner, across, beyond]
    own_weights = [weight(own, q) for q in sources]
    line_weights = [[weight(p, q) for q in sources] for p in columns]
    part_step = LARGEST * 4.0 / pops / LEVELS
    cost_step = LARGEST / LEVELS

    def coded(x, step):
        return jnp.round(x * (1.0 / step)).astype(jnp.int32).astype(jnp.int16)

    def decoded(x, step):
        return x.astype(jnp.int32).astype(jnp.float32) * step

    def stage_relay(n):
        t = steps - 1 - n
        arrived(near.at[1, t], near_recv.at[1, n])
        sent.append(remote(near.at[1, t], near.at[2, t], near_send.at[2, n], near_recv.at[2, n], {"pop": partner}))

    def stage_partial(n):
        t = steps - 1 - n
        arrived(near.at[0, t], near_recv.at[0, n])
        arrived(near.at[2, t], near_recv.at[2, n])
        for c in range(0, cols, CHUNK):
            span = slice(c, c + CHUNK)
            blocks = [history[t, :, span], near[0, t, :, span], near[1, t, :, span], near[2, t, :, span]]
            blocks = [b.astype(jnp.float32) - CENTRE for b in blocks]

            def mixed(factors):
                total = factors[0] * blocks[0]
                for f, b in zip(factors[1:], blocks[1:]):
                    total = total + f * b
                return total

            for j in range(outer - 1):
                part_out[j, n, :, span] = coded(mixed(line_weights[j]), part_step)
            own_sum[n, :, span] = mixed(own_weights)
        for j, q in enumerate(columns):
            sent.append(remote(part_out.at[j, n], part_in.at[j, n], part_send.at[j, n], part_recv.at[j, n], {"pop": q}))

    def stage_total(n):
        total = own_sum[n]
        for j in range(outer - 1):
            arrived(part_in.at[j, n], part_recv.at[j, n])
            total = total + decoded(part_in[j, n], part_step)
        for z in range(tiles):
            cost_out[n, z, :, :width] = coded(main_of(total, z), cost_step)
            cost_out[n, z, :, width:] = coded(rim_of(total, z), cost_step)
        spread(cost_out.at[n], cost_in.at[n], cost_send.at[n], cost_recv.at[n])
        cost_in[n, me] = cost_out[n, me]

    def ahead_r(x):
        return pltpu.roll(x, total_rows - 1, 0)

    def behind_r(x):
        return pltpu.roll(x, 1, 0)

    def ahead_c(x):
        return pltpu.roll(x, full - 1, 1)

    def behind_c(x):
        return pltpu.roll(x, 1, 1)

    def send_back(src, dst, n):
        pltpu.make_async_copy(src.at[me], dst.at[:, cut(me)], back_self.at[n]).start()
        for z in peers:
            remote(src.at[z], dst.at[:, cut(me)], back_send.at[n], back_recv.at[n], {"tile": z})

    def wait_back(src, dst, n):
        pltpu.make_async_copy(src.at[me], dst.at[:, cut(me)], back_self.at[n]).wait()
        landed = dst.at[:, pl.ds(0, (tiles - 1) * width)]
        arrived(landed, back_recv.at[n])
        arrived(landed, back_send.at[n])

    state = {}

    def stage_sweep(n):
        t = steps - 1 - n
        if n == 0:
            wait_spread(start_value, start_recv.at[0])
            state["u"] = start_value[...].reshape(total_rows, full)
        wait_spread(cost_in.at[n], cost_recv.at[n])
        source = decoded(cost_in[n], cost_step).reshape(total_rows, full)
        u = state["u"]
        dr = ahead_r(u) - u
        dc = ahead_c(u) - u
        if t + 1 < steps:
            slope_r[t + 1] = dr
            slope_c[t + 1] = dc
        er, ec = behind_r(dr), behind_c(dc)
        br, bc = jnp.maximum(er, 0.0), jnp.maximum(ec, 0.0)
        ar, ac = jnp.minimum(dr, 0.0), jnp.minimum(dc, 0.0)
        lap = (dr - er) + (dc - ec)
        ham = 0.5 * ((br * br + ar * ar) + (bc * bc + ac * ac))
        u = u + time_step * (viscosity * lap - ham + source)
        state["u"] = u
        main = u[:, :width]
        swept[t] = main.reshape(tiles, rows, width)
        send_back(swept.at[t], values.at[t], t)
        line_sum = jnp.sum(main, axis=0, keepdims=True)
        folded = line_sum[:, :LANES]
        for j in range(1, width // LANES):
            folded = folded + line_sum[:, j * LANES:(j + 1) * LANES]
        sums_own[t:t + 1, :] = folded

    stages = [(RELAY, stage_relay), (PARTIAL, stage_partial), (TOTAL, stage_total), (SWEEP, stage_sweep)]
    plan = sorted((first + per * n, k, n) for k, ((first, per), _) in enumerate(stages) for n in range(steps))
    for _, k, n in plan:
        stages[k][1](n)

    sums_n = steps + 1
    sums_all[me] = sums_own[...]
    for z in peers:
        remote(sums_own, sums_all.at[me], back_send.at[sums_n], back_recv.at[sums_n], {"tile": z})

    wait_spread(start_mass, start_recv.at[1])
    u = state["u"]
    mass = start_mass[...].reshape(total_rows, full)
    for t in range(steps):
        if t == 0:
            dr, dc = ahead_r(u) - u, ahead_c(u) - u
        else:
            dr, dc = slope_r[t], slope_c[t]
        mr, mc = ahead_r(mass), ahead_c(mass)
        flux_r = jnp.maximum(-dr, 0.0) * mass + jnp.minimum(-dr, 0.0) * mr
        flux_c = jnp.maximum(-dc, 0.0) * mass + jnp.minimum(-dc, 0.0) * mc
        net_r = viscosity * (mr - mass) - flux_r
        net_c = viscosity * (mc - mass) - flux_c
        mass = mass + time_step * ((net_r - behind_r(net_r)) + (net_c - behind_c(net_c)))
    mass_main[...] = mass[:, :width].reshape(tiles, rows, width)
    send_back(mass_main, density_out, steps)

    arrived(sums_all.at[pl.ds(0, tiles - 1)], back_recv.at[sums_n])
    arrived(sums_all.at[pl.ds(0, tiles - 1)], back_send.at[sums_n])
    grand = jnp.sum(jnp.sum(sums_all[...], axis=0), axis=1, keepdims=True) * (1.0 / (total_rows * cols))
    for t in reversed(range(steps)):
        wait_back(swept.at[t], values.at[t], t)
        values[t] = values[t] - grand[t:t + 1, :]
    wait_back(mass_main, density_out, steps)
    wait_spread(start_value, start_send.at[0])
    wait_spread(start_mass, start_send.at[1])
    for n in range(steps):
        wait_spread(cost_in.at[n], cost_send.at[n])
    for copy in sent:
        copy.wait_send()


def finish(values, density, values_out, density_out, sems):
    copies = [
        pltpu.make_async_copy(values, values_out, sems.at[0]),
        pltpu.make_async_copy(density, density_out, sems.at[1]),
    ]
    for copy in copies:
        copy.start()
    for copy in copies:
        copy.wait()


def per_device(pops, tiles, weights, terminal, density_history, density_init):
    _, steps, rows, cols = density_history.shape
    width = cols // tiles
    outer = pops // 4
    total_rows = tiles * rows
    full = width + LANES
    dma = pltpu.SemaphoreType.DMA
    lines = max(outer - 1, 1)
    vmem = pl.BlockSpec(memory_space=pltpu.VMEM)
    anywhere = pl.BlockSpec(memory_space=pl.ANY)
    values, density = pl.pallas_call(
        functools.partial(kernel, pops, tiles),
        out_shape=(
            pltpu.VMEM((steps, rows, cols), jnp.float32),
            pltpu.VMEM((rows, cols), jnp.float32),
        ),
        in_specs=[pl.BlockSpec(memory_space=pltpu.SMEM), anywhere, anywhere, anywhere],
        out_specs=(vmem, vmem),
        scratch_shapes=[
            pltpu.VMEM((rows, cols), jnp.float32),
            pltpu.VMEM((steps, rows, cols), jnp.bfloat16),
            pltpu.VMEM((rows, cols), jnp.float32),
            dma((3,)),
            pltpu.VMEM((3, steps, rows, cols), jnp.bfloat16),
            pltpu.VMEM((steps, rows, cols), jnp.float32),
            pltpu.VMEM((lines, steps, rows, cols), jnp.int16),
            pltpu.VMEM((lines, steps, rows, cols), jnp.int16),
            pltpu.VMEM((steps, tiles, rows, full), jnp.int16),
            pltpu.VMEM((steps, tiles, rows, full), jnp.int16),
            pltpu.VMEM((tiles, rows, full), jnp.float32),
            pltpu.VMEM((tiles, rows, full), jnp.float32),
            pltpu.VMEM((tiles, rows, full), jnp.float32),
            pltpu.VMEM((tiles, rows, full), jnp.float32),
            pltpu.VMEM((steps, tiles, rows, width), jnp.float32),
            pltpu.VMEM((tiles, rows, width), jnp.float32),
            pltpu.VMEM((steps, total_rows, full), jnp.float32),
            pltpu.VMEM((steps, total_rows, full), jnp.float32),
            pltpu.VMEM((steps, LANES), jnp.float32),
            pltpu.VMEM((tiles, steps, LANES), jnp.float32),
            dma((3, steps)), dma((3, steps)),
            dma((lines, steps)), dma((lines, steps)),
            dma((steps,)), dma((steps,)),
            dma((2,)), dma((2,)),
            dma((steps + 2,)), dma((steps + 2,)), dma((steps + 1,)),
        ],
        compiler_params=pltpu.CompilerParams(collective_id=0, has_side_effects=True),
    )(weights, terminal[0], density_history[0], density_init[0])
    values, density = pl.pallas_call(
        finish,
        out_shape=(
            jax.ShapeDtypeStruct((steps, rows, cols), jnp.float32),
            jax.ShapeDtypeStruct((rows, cols), jnp.float32),
        ),
        in_specs=[anywhere, anywhere],
        out_specs=(anywhere, anywhere),
        scratch_shapes=[dma((2,))],
        compiler_params=pltpu.CompilerParams(vmem_limit_bytes=8 * 1024 * 1024),
    )(values, density)
    return values[None], density[None]


def solution(mesh):
    in_specs = (P(), P("pop", "tile", None), P("pop", None, "tile", None), P("pop", "tile", None))
    out_specs = (P("pop", None, "tile", None), P("pop", "tile", None))
    body = functools.partial(per_device, mesh.shape["pop"], mesh.shape["tile"])
    return jax.shard_map(body, mesh=mesh, in_specs=in_specs, out_specs=out_specs, check_vma=False)
```

```python
import functools

import jax
import jax.numpy as jnp
from jax import lax
from jax.experimental import pallas as pl
from jax.experimental.pallas import tpu as pltpu
from jax.sharding import PartitionSpec as P

time_step = 0.2
viscosity = 0.2
LANES = 128
CHUNK = 512
CENTRE = 1.1
LARGEST = 3.0 * 0.901
LEVELS = 32400.0
RELAY = (2.6, 0.65)
PARTIAL = (3.6, 0.65)
TOTAL = (6.5, 0.65)
SWEEP = (10.3, 0.65)
STRIP = (14.0, 0.65)


def kernel(pops, tiles, weights_in, terminal_in, history_in, initial_in, values, density_out,
           weights, terminal, history, initial, load_sem, near, own_sum, part_out, part_in, cost_out, cost_in,
           value_out, start_value, mass_out, start_mass, edge_out, edge_in, mass_main, slope_r, slope_c, sums_own, sums_all,
           near_send, near_recv, part_send, part_recv, cost_send, cost_recv, start_send, start_recv,
           edge_send, edge_recv, back_send, back_recv, back_self):
    steps, rows, cols = history.shape
    width = cols // tiles
    full = width + LANES
    total_rows = tiles * rows
    outer = pops // 4
    me = lax.axis_index("tile")
    own = lax.axis_index("pop")
    core = own % 2
    plane = (own // 2) % 2
    line = own // 4

    def pop_of(a, b, c):
        return (a * 2 + b) * 2 + c

    partner = pop_of(line, plane, 1 - core)
    across = pop_of(line, 1 - plane, core)
    beyond = pop_of(line, 1 - plane, 1 - core)
    columns = [pop_of((line + j) % outer, plane, core) for j in range(1, outer)]
    peers = [(me + d) % tiles for d in range(1, tiles)]

    barrier = pltpu.get_barrier_semaphore()
    greeted = [{"tile": z} for z in peers] + [{"pop": q} for q in [partner, across] + columns]
    for there in greeted:
        pl.semaphore_signal(barrier, inc=1, device_id=there, device_id_type=pl.DeviceIdType.MESH)

    loads = [pltpu.make_async_copy(src, dst, load_sem.at[n]) for n, (src, dst) in enumerate(
        [(weights_in, weights), (terminal_in, terminal), (initial_in, initial), (history_in, history)])]
    for load in loads:
        load.start()
    for load in loads:
        load.wait()
    right_side = lax.broadcasted_iota(jnp.int32, (rows, LANES), 1) < LANES // 2

    def main_of(block, z):
        return block[:, z * width:(z + 1) * width]

    def rim_of(block, z):
        right = ((z + 1) % tiles) * width
        left = ((z + tiles - 1) % tiles) * width + width - LANES
        return jnp.where(right_side, block[:, right:right + LANES], block[:, left:left + LANES])

    for src, dst in [(terminal, value_out), (initial, mass_out)]:
        block = src[...]
        for z in range(tiles):
            dst[z, :, :width] = main_of(block, z)
            dst[z, :, width:] = rim_of(block, z)
    start_value[me] = value_out[me]
    start_mass[me] = mass_out[me]

    pl.semaphore_wait(barrier, len(greeted))

    def cut(z):
        return pl.ds(pl.multiple_of(z * width, LANES), width)

    sent = []

    def remote(src, dst, send, recv, there):
        copy = pltpu.make_async_remote_copy(src_ref=src, dst_ref=dst, send_sem=send, recv_sem=recv,
                                            device_id=there, device_id_type=pl.DeviceIdType.MESH)
        copy.start()
        return copy

    def arrived(ref, sem):
        pltpu.make_async_copy(ref, ref, sem).wait()

    def spread(src, dst, send, recv):
        for z in peers:
            remote(src.at[z], dst.at[me], send, recv, {"tile": z})

    def wait_spread(dst, sem):
        arrived(dst.at[pl.ds(0, tiles - 1)], sem)

    for n in range(steps):
        t = steps - 1 - n
        sent.append(remote(history.at[t], near.at[1, t], near_send.at[1, n], near_recv.at[1, n], {"pop": across}))
        sent.append(remote(history.at[t], near.at[0, t], near_send.at[0, n], near_recv.at[0, n], {"pop": partner}))
    spread(value_out, start_value, start_send.at[0], start_recv.at[0])
    spread(mass_out, start_mass, start_send.at[1], start_recv.at[1])

    def weight(p, q):
        return weights[p, q].astype(jnp.float32) * (1.0 / pops)

    sources = [own, partner, across, beyond]
    own_weights = [weight(own, q) for q in sources]
    line_weights = [[weight(p, q) for q in sources] for p in columns]
    part_step = LARGEST * 4.0 / pops / LEVELS
    cost_step = LARGEST / LEVELS

    def coded(x, step):
        return jnp.round(x * (1.0 / step)).astype(jnp.int32).astype(jnp.int16)

    def decoded(x, step):
        return x.astype(jnp.int32).astype(jnp.float32) * step

    def stage_relay(n):
        t = steps - 1 - n
        arrived(near.at[1, t], near_recv.at[1, n])
        sent.append(remote(near.at[1, t], near.at[2, t], near_send.at[2, n], near_recv.at[2, n], {"pop": partner}))

    def stage_partial(n):
        t = steps - 1 - n
        arrived(near.at[0, t], near_recv.at[0, n])
        arrived(near.at[2, t], near_recv.at[2, n])
        for c in range(0, cols, CHUNK):
            span = slice(c, c + CHUNK)
            blocks = [history[t, :, span], near[0, t, :, span], near[1, t, :, span], near[2, t, :, span]]
            blocks = [b.astype(jnp.float32) - CENTRE for b in blocks]

            def mixed(factors):
                total = factors[0] * blocks[0]
                for f, b in zip(factors[1:], blocks[1:]):
                    total = total + f * b
                return total

            for j in range(outer - 1):
                part_out[j, n, :, span] = coded(mixed(line_weights[j]), part_step)
            own_sum[n, :, span] = mixed(own_weights)
        for j, q in enumerate(columns):
            sent.append(remote(part_out.at[j, n], part_in.at[j, n], part_send.at[j, n], part_recv.at[j, n], {"pop": q}))

    def stage_total(n):
        total = own_sum[n]
        for j in range(outer - 1):
            arrived(part_in.at[j, n], part_recv.at[j, n])
            total = total + decoded(part_in[j, n], part_step)
        own_sum[n] = total
        for z in range(tiles):
            cost_out[n, z, :, :width] = coded(main_of(total, z), cost_step)
            cost_out[n, z, :, width:] = coded(rim_of(total, z), cost_step)
        spread(cost_out.at[n], cost_in.at[n], cost_send.at[n], cost_recv.at[n])
        cost_in[n, me] = cost_out[n, me]

    def ahead_r(x):
        return pltpu.roll(x, total_rows - 1, 0)

    def behind_r(x):
        return pltpu.roll(x, 1, 0)

    def ahead_c(x):
        return pltpu.roll(x, full - 1, 1)

    def behind_c(x):
        return pltpu.roll(x, 1, 1)

    def send_edges(main, n):
        for z in range(tiles):
            above = (z * rows + total_rows - 1) % total_rows
            below = (z * rows + rows) % total_rows
            edge_out[n, z, 0:1, :] = main[above:above + 1, :]
            edge_out[n, z, 1:2, :] = main[below:below + 1, :]
        spread(edge_out.at[n], edge_in.at[n], edge_send.at[n], edge_recv.at[n])
        edge_in[n, me] = edge_out[n, me]

    def send_back(src, dst, n):
        pltpu.make_async_copy(src.at[me], dst.at[:, cut(me)], back_self.at[n]).start()
        for z in peers:
            remote(src.at[z], dst.at[:, cut(me)], back_send.at[n], back_recv.at[n], {"tile": z})

    def wait_back(src, dst, n):
        pltpu.make_async_copy(src.at[me], dst.at[:, cut(me)], back_self.at[n]).wait()
        landed = dst.at[:, pl.ds(0, (tiles - 1) * width)]
        arrived(landed, back_recv.at[n])
        arrived(landed, back_send.at[n])

    state = {}

    def stage_sweep(n):
        t = steps - 1 - n
        if n == 0:
            wait_spread(start_value, start_recv.at[0])
            state["u"] = start_value[...].reshape(total_rows, full)
            send_edges(state["u"][:, :width], 0)
        wait_spread(cost_in.at[n], cost_recv.at[n])
        source = decoded(cost_in[n], cost_step).reshape(total_rows, full)
        u = state["u"]
        dr = ahead_r(u) - u
        dc = ahead_c(u) - u
        if t + 1 < steps:
            slope_r[t + 1] = dr
            slope_c[t + 1] = dc
        er, ec = behind_r(dr), behind_c(dc)
        br, bc = jnp.maximum(er, 0.0), jnp.maximum(ec, 0.0)
        ar, ac = jnp.minimum(dr, 0.0), jnp.minimum(dc, 0.0)
        lap = (dr - er) + (dc - ec)
        ham = 0.5 * ((br * br + ar * ar) + (bc * bc + ac * ac))
        u = u + time_step * (viscosity * lap - ham + source)
        state["u"] = u
        main = u[:, :width]
        if t > 0:
            send_edges(main, n + 1)
        line_sum = jnp.sum(main, axis=0, keepdims=True)
        folded = line_sum[:, :LANES]
        for j in range(1, width // LANES):
            folded = folded + line_sum[:, j * LANES:(j + 1) * LANES]
        sums_own[t:t + 1, :] = folded

    row = lax.broadcasted_iota(jnp.int32, (rows, cols), 0)

    def stage_strip(n):
        t = steps - 1 - n
        wait_spread(edge_in.at[n], edge_recv.at[n])
        above = jnp.concatenate([edge_in[n, z, 0:1, :] for z in range(tiles)], axis=1)
        below = jnp.concatenate([edge_in[n, z, 1:2, :] for z in range(tiles)], axis=1)
        u = terminal[...] if n == 0 else values[t + 1]
        dr = jnp.where(row == rows - 1, below, pltpu.roll(u, rows - 1, 0)) - u
        er = u - jnp.where(row == 0, above, pltpu.roll(u, 1, 0))
        dc = pltpu.roll(u, cols - 1, 1) - u
        ec = pltpu.roll(dc, 1, 1)
        br, bc = jnp.maximum(er, 0.0), jnp.maximum(ec, 0.0)
        ar, ac = jnp.minimum(dr, 0.0), jnp.minimum(dc, 0.0)
        lap = (dr - er) + (dc - ec)
        ham = 0.5 * ((br * br + ar * ar) + (bc * bc + ac * ac))
        values[t] = u + time_step * (viscosity * lap - ham + own_sum[n])

    stages = [(RELAY, stage_relay), (PARTIAL, stage_partial), (TOTAL, stage_total), (SWEEP, stage_sweep), (STRIP, stage_strip)]
    plan = sorted((first + per * n, k, n) for k, ((first, per), _) in enumerate(stages) for n in range(steps))
    last = plan.index((SWEEP[0] + SWEEP[1] * (steps - 1), 3, steps - 1)) + 1
    for _, k, n in plan[:last]:
        stages[k][1](n)

    sums_n = 1
    sums_all[me] = sums_own[...]
    for z in peers:
        remote(sums_own, sums_all.at[me], back_send.at[sums_n], back_recv.at[sums_n], {"tile": z})

    wait_spread(start_mass, start_recv.at[1])
    u = state["u"]
    mass = start_mass[...].reshape(total_rows, full)
    for t in range(steps):
        if t == 0:
            dr, dc = ahead_r(u) - u, ahead_c(u) - u
        else:
            dr, dc = slope_r[t], slope_c[t]
        mr, mc = ahead_r(mass), ahead_c(mass)
        flux_r = jnp.maximum(-dr, 0.0) * mass + jnp.minimum(-dr, 0.0) * mr
        flux_c = jnp.maximum(-dc, 0.0) * mass + jnp.minimum(-dc, 0.0) * mc
        net_r = viscosity * (mr - mass) - flux_r
        net_c = viscosity * (mc - mass) - flux_c
        mass = mass + time_step * ((net_r - behind_r(net_r)) + (net_c - behind_c(net_c)))
    mass_main[...] = mass[:, :width].reshape(tiles, rows, width)
    send_back(mass_main, density_out, 0)
    for _, k, n in plan[last:]:
        stages[k][1](n)

    arrived(sums_all.at[pl.ds(0, tiles - 1)], back_recv.at[sums_n])
    arrived(sums_all.at[pl.ds(0, tiles - 1)], back_send.at[sums_n])
    grand = jnp.sum(jnp.sum(sums_all[...], axis=0), axis=1, keepdims=True) * (1.0 / (total_rows * cols))
    for t in reversed(range(steps)):
        values[t] = values[t] - grand[t:t + 1, :]
    wait_back(mass_main, density_out, 0)
    wait_spread(start_value, start_send.at[0])
    wait_spread(start_mass, start_send.at[1])
    for n in range(steps):
        wait_spread(cost_in.at[n], cost_send.at[n])
        wait_spread(edge_in.at[n], edge_send.at[n])
    for copy in sent:
        copy.wait_send()


def finish(values, density, values_out, density_out, sems):
    copies = [
        pltpu.make_async_copy(values, values_out, sems.at[0]),
        pltpu.make_async_copy(density, density_out, sems.at[1]),
    ]
    for copy in copies:
        copy.start()
    for copy in copies:
        copy.wait()


def per_device(pops, tiles, weights, terminal, density_history, density_init):
    _, steps, rows, cols = density_history.shape
    width = cols // tiles
    outer = pops // 4
    total_rows = tiles * rows
    full = width + LANES
    dma = pltpu.SemaphoreType.DMA
    lines = max(outer - 1, 1)
    vmem = pl.BlockSpec(memory_space=pltpu.VMEM)
    anywhere = pl.BlockSpec(memory_space=pl.ANY)
    values, density = pl.pallas_call(
        functools.partial(kernel, pops, tiles),
        out_shape=(
            pltpu.VMEM((steps, rows, cols), jnp.float32),
            pltpu.VMEM((rows, cols), jnp.float32),
        ),
        in_specs=[anywhere, anywhere, anywhere, anywhere],
        out_specs=(vmem, vmem),
        scratch_shapes=[
            pltpu.SMEM((pops, pops), jnp.int32),
            pltpu.VMEM((rows, cols), jnp.float32),
            pltpu.VMEM((steps, rows, cols), jnp.bfloat16),
            pltpu.VMEM((rows, cols), jnp.float32),
            dma((4,)),
            pltpu.VMEM((3, steps, rows, cols), jnp.bfloat16),
            pltpu.VMEM((steps, rows, cols), jnp.float32),
            pltpu.VMEM((lines, steps, rows, cols), jnp.int16),
            pltpu.VMEM((lines, steps, rows, cols), jnp.int16),
            pltpu.VMEM((steps, tiles, rows, full), jnp.int16),
            pltpu.VMEM((steps, tiles, rows, full), jnp.int16),
            pltpu.VMEM((tiles, rows, full), jnp.float32),
            pltpu.VMEM((tiles, rows, full), jnp.float32),
            pltpu.VMEM((tiles, rows, full), jnp.float32),
            pltpu.VMEM((tiles, rows, full), jnp.float32),
            pltpu.VMEM((steps, tiles, 2, width), jnp.float32),
            pltpu.VMEM((steps, tiles, 2, width), jnp.float32),
            pltpu.VMEM((tiles, rows, width), jnp.float32),
            pltpu.VMEM((steps, total_rows, full), jnp.float32),
            pltpu.VMEM((steps, total_rows, full), jnp.float32),
            pltpu.VMEM((steps, LANES), jnp.float32),
            pltpu.VMEM((tiles, steps, LANES), jnp.float32),
            dma((3, steps)), dma((3, steps)),
            dma((lines, steps)), dma((lines, steps)),
            dma((steps,)), dma((steps,)),
            dma((2,)), dma((2,)),
            dma((steps,)), dma((steps,)),
            dma((2,)), dma((2,)), dma((1,)),
        ],
        compiler_params=pltpu.CompilerParams(collective_id=0, has_side_effects=True),
    )(weights, terminal[0], density_history[0], density_init[0])
    values, density = pl.pallas_call(
        finish,
        out_shape=(
            jax.ShapeDtypeStruct((steps, rows, cols), jnp.float32),
            jax.ShapeDtypeStruct((rows, cols), jnp.float32),
        ),
        in_specs=[anywhere, anywhere],
        out_specs=(anywhere, anywhere),
        scratch_shapes=[dma((2,))],
        compiler_params=pltpu.CompilerParams(vmem_limit_bytes=8 * 1024 * 1024),
    )(values, density)
    return values[None], density[None]


def solution(mesh):
    in_specs = (P(), P("pop", "tile", None), P("pop", None, "tile", None), P("pop", "tile", None))
    out_specs = (P("pop", None, "tile", None), P("pop", "tile", None))
    body = functools.partial(per_device, mesh.shape["pop"], mesh.shape["tile"])
    return jax.shard_map(body, mesh=mesh, in_specs=in_specs, out_specs=out_specs, check_vma=False)
```

```python
import functools

import jax
import jax.numpy as jnp
from jax import lax
from jax.experimental import pallas as pl
from jax.experimental.pallas import tpu as pltpu
from jax.sharding import PartitionSpec as P

time_step = 0.2
viscosity = 0.2
LANES = 128
WINDOWS = 4
SPAN = LANES // WINDOWS
CHUNK = 512
CENTRE = 1.1
LARGEST = 3.0 * 0.901
LEVELS = 32400.0
RELAY = (2.6, 0.35)
PARTIAL = (3.6, 0.35)
TOTAL = (6.4, 0.6)
SWEEP = (12.5, 0.9)
STRIP = (20.0, 0.65)


def kernel(pops, tiles, weights_in, terminal_in, history_in, initial_in, values, density_out,
           weights, terminal, history, initial, load_sem, near_other, near, near_relay, own_sum, part_out, part_in,
           cost_out, cost_in, rim_out, rim_in, value_out, start_value, mass_out, start_mass, edge_out, edge_in, mass_main, slope_r, slope_c, sums_own, sums_all,
           other_send, other_recv, near_send, near_recv, relay_send, relay_recv, part_send, part_recv,
           cost_send, cost_recv, rim_send, rim_recv, start_send, start_recv,
           edge_send, edge_recv, back_send, back_recv, back_self):
    steps, rows, cols = history.shape
    width = cols // tiles
    full = width + LANES
    total_rows = tiles * rows
    outer = pops // 4
    me = lax.axis_index("tile")
    own = lax.axis_index("pop")
    core = own % 2
    plane = (own // 2) % 2
    line = own // 4

    def pop_of(a, b, c):
        return (a * 2 + b) * 2 + c

    partner = pop_of(line, plane, 1 - core)
    across = pop_of(line, 1 - plane, core)
    columns = [pop_of((line + j) % outer, plane, core) for j in range(1, outer)]
    behind = [(line + outer - j) % outer for j in range(1, outer)]

    def along_row(n):
        return n % 2 == 0 or outer == 1

    def first_peers(n):
        return [across] if along_row(n) else columns

    def second_peers(n):
        return columns if along_row(n) else [across]

    def sources(n):
        far = [(line, 1 - plane)] if along_row(n) else [(a, plane) for a in behind]
        return [own, partner] + [pop_of(a, b, core) for a, b in far] + [pop_of(a, b, 1 - core) for a, b in far]

    peers = [(me + d) % tiles for d in range(1, tiles)]

    barrier = pltpu.get_barrier_semaphore()
    greeted = [{"tile": z} for z in peers] + [{"pop": q} for q in [partner, across] + columns]
    for there in greeted:
        pl.semaphore_signal(barrier, inc=1, device_id=there, device_id_type=pl.DeviceIdType.MESH)

    loads = [pltpu.make_async_copy(src, dst, load_sem.at[n]) for n, (src, dst) in enumerate(
        [(weights_in, weights), (terminal_in, terminal), (initial_in, initial), (history_in, history)])]
    for load in loads:
        load.start()
    for load in loads:
        load.wait()
    lane = lax.broadcasted_iota(jnp.int32, (rows, LANES), 1)
    window = ((lane + SPAN // 2) % LANES) // SPAN
    right_side = lax.broadcasted_iota(jnp.int32, (rows, LANES), 1) < LANES // 2

    def main_of(block, z):
        return block[:, z * width:(z + 1) * width]

    def rim_of(block, z):
        right = ((z + 1) % tiles) * width
        left = ((z + tiles - 1) % tiles) * width + width - LANES
        return jnp.where(right_side, block[:, right:right + LANES], block[:, left:left + LANES])

    for src, dst in [(terminal, value_out), (initial, mass_out)]:
        block = src[...]
        for z in range(tiles):
            dst[z, :, :width] = main_of(block, z)
            dst[z, :, width:] = rim_of(block, z)
    start_value[me] = value_out[me]
    start_mass[me] = mass_out[me]

    pl.semaphore_wait(barrier, len(greeted))

    def cut(z):
        return pl.ds(pl.multiple_of(z * width, LANES), width)

    sent = []

    def remote(src, dst, send, recv, there):
        copy = pltpu.make_async_remote_copy(src_ref=src, dst_ref=dst, send_sem=send, recv_sem=recv,
                                            device_id=there, device_id_type=pl.DeviceIdType.MESH)
        copy.start()
        return copy

    def arrived(ref, sem):
        pltpu.make_async_copy(ref, ref, sem).wait()

    def spread(src, dst, send, recv):
        for z in peers:
            remote(src.at[z], dst.at[me], send, recv, {"tile": z})

    def wait_spread(dst, sem):
        arrived(dst.at[pl.ds(0, tiles - 1)], sem)

    for n in range(steps):
        t = steps - 1 - n
        for j, q in enumerate(first_peers(n)):
            sent.append(remote(history.at[t], near.at[j, t], near_send.at[j, n], near_recv.at[j, n], {"pop": q}))
        sent.append(remote(history.at[t], near_other.at[t], other_send.at[n], other_recv.at[n], {"pop": partner}))
    spread(value_out, start_value, start_send.at[0], start_recv.at[0])
    spread(mass_out, start_mass, start_send.at[1], start_recv.at[1])

    def weight(p, q):
        return weights[p, q].astype(jnp.float32) * (1.0 / pops)

    def part_step(n):
        return LARGEST * (4.0 if along_row(n) else 2.0 * outer) / pops / LEVELS

    cost_step = LARGEST / LEVELS

    def coded(x, step):
        return jnp.round(x * (1.0 / step)).astype(jnp.int32).astype(jnp.int16)

    def decoded(x, step):
        return x.astype(jnp.int32).astype(jnp.float32) * step

    def stage_relay(n):
        t = steps - 1 - n
        for j in range(len(first_peers(n))):
            arrived(near.at[j, t], near_recv.at[j, n])
            sent.append(remote(near.at[j, t], near_relay.at[j, t], relay_send.at[j, n], relay_recv.at[j, n],
                               {"pop": partner}))

    def stage_partial(n):
        t = steps - 1 - n
        far = range(len(first_peers(n)))
        arrived(near_other.at[t], other_recv.at[n])
        for j in far:
            arrived(near_relay.at[j, t], relay_recv.at[j, n])
        own_factors = [weight(own, q) for q in sources(n)]
        part_factors = [[weight(p, q) for q in sources(n)] for p in second_peers(n)]
        for c in range(0, cols, CHUNK):
            span = slice(c, c + CHUNK)
            blocks = [history[t, :, span], near_other[t, :, span]]
            blocks += [near[j, t, :, span] for j in far] + [near_relay[j, t, :, span] for j in far]
            blocks = [b.astype(jnp.float32) - CENTRE for b in blocks]

            def mixed(factors):
                total = factors[0] * blocks[0]
                for f, b in zip(factors[1:], blocks[1:]):
                    total = total + f * b
                return total

            for j, factors in enumerate(part_factors):
                part_out[j, n, :, span] = coded(mixed(factors), part_step(n))
            own_sum[n, :, span] = mixed(own_factors)
        for j, q in enumerate(second_peers(n)):
            sent.append(remote(part_out.at[j, n], part_in.at[j, n], part_send.at[j, n], part_recv.at[j, n], {"pop": q}))

    def stage_total(n):
        total = own_sum[n]
        for j in range(len(second_peers(n))):
            arrived(part_in.at[j, n], part_recv.at[j, n])
            total = total + decoded(part_in[j, n], part_step(n))
        own_sum[n] = total
        for z in range(tiles):
            cost_out[n, z] = coded(main_of(total, z), cost_step)
        spread(cost_out.at[n], cost_in.at[n], cost_send.at[n], cost_recv.at[n])
        cost_in[n, me] = cost_out[n, me]
        g, k = n // WINDOWS, n % WINDOWS
        if k == WINDOWS - 1:
            for z in range(tiles):
                rim = rim_of(own_sum[g * WINDOWS], z)
                for i in range(1, WINDOWS):
                    rim = jnp.where(window == i, pltpu.roll(rim_of(own_sum[g * WINDOWS + i], z), SPAN * i, 1), rim)
                rim_out[g, z] = coded(rim, cost_step)
            spread(rim_out.at[g], rim_in.at[g], rim_send.at[g], rim_recv.at[g])
            rim_in[g, me] = rim_out[g, me]

    def ahead_r(x):
        return pltpu.roll(x, total_rows - 1, 0)

    def behind_r(x):
        return pltpu.roll(x, 1, 0)

    def ahead_c(x):
        return pltpu.roll(x, full - 1, 1)

    def behind_c(x):
        return pltpu.roll(x, 1, 1)

    def send_edges(main, n):
        for z in range(tiles):
            above = (z * rows + total_rows - 1) % total_rows
            below = (z * rows + rows) % total_rows
            edge_out[n, z, 0:1, :] = main[above:above + 1, :]
            edge_out[n, z, 1:2, :] = main[below:below + 1, :]
        spread(edge_out.at[n], edge_in.at[n], edge_send.at[n], edge_recv.at[n])
        edge_in[n, me] = edge_out[n, me]

    def send_back(src, dst, n):
        pltpu.make_async_copy(src.at[me], dst.at[:, cut(me)], back_self.at[n]).start()
        for z in peers:
            remote(src.at[z], dst.at[:, cut(me)], back_send.at[n], back_recv.at[n], {"tile": z})

    def wait_back(src, dst, n):
        pltpu.make_async_copy(src.at[me], dst.at[:, cut(me)], back_self.at[n]).wait()
        landed = dst.at[:, pl.ds(0, (tiles - 1) * width)]
        arrived(landed, back_recv.at[n])
        arrived(landed, back_send.at[n])

    state = {}

    def stage_sweep(n):
        t = steps - 1 - n
        if n == 0:
            wait_spread(start_value, start_recv.at[0])
            state["u"] = start_value[...].reshape(total_rows, full)
            send_edges(state["u"][:, :width], 0)
        wait_spread(cost_in.at[n], cost_recv.at[n])
        g, k = n // WINDOWS, n % WINDOWS
        if k == 0:
            wait_spread(rim_in.at[g], rim_recv.at[g])
            state["rim"] = decoded(rim_in[g], cost_step).reshape(total_rows, LANES)
        rim = state["rim"] if k == 0 else pltpu.roll(state["rim"], LANES - SPAN * k, 1)
        source = jnp.concatenate([decoded(cost_in[n], cost_step).reshape(total_rows, width), rim], axis=1)
        u = state["u"]
        dr = ahead_r(u) - u
        dc = ahead_c(u) - u
        if t + 1 < steps:
            slope_r[t + 1] = dr
            slope_c[t + 1] = dc
        er, ec = behind_r(dr), behind_c(dc)
        br, bc = jnp.maximum(er, 0.0), jnp.maximum(ec, 0.0)
        ar, ac = jnp.minimum(dr, 0.0), jnp.minimum(dc, 0.0)
        lap = (dr - er) + (dc - ec)
        ham = 0.5 * ((br * br + ar * ar) + (bc * bc + ac * ac))
        u = u + time_step * (viscosity * lap - ham + source)
        state["u"] = u
        main = u[:, :width]
        if t > 0:
            send_edges(main, n + 1)
        line_sum = jnp.sum(main, axis=0, keepdims=True)
        folded = line_sum[:, :LANES]
        for j in range(1, width // LANES):
            folded = folded + line_sum[:, j * LANES:(j + 1) * LANES]
        sums_own[t:t + 1, :] = folded

    row = lax.broadcasted_iota(jnp.int32, (rows, cols), 0)

    def stage_strip(n):
        t = steps - 1 - n
        wait_spread(edge_in.at[n], edge_recv.at[n])
        above = jnp.concatenate([edge_in[n, z, 0:1, :] for z in range(tiles)], axis=1)
        below = jnp.concatenate([edge_in[n, z, 1:2, :] for z in range(tiles)], axis=1)
        u = terminal[...] if n == 0 else values[t + 1]
        dr = jnp.where(row == rows - 1, below, pltpu.roll(u, rows - 1, 0)) - u
        er = u - jnp.where(row == 0, above, pltpu.roll(u, 1, 0))
        dc = pltpu.roll(u, cols - 1, 1) - u
        ec = pltpu.roll(dc, 1, 1)
        br, bc = jnp.maximum(er, 0.0), jnp.maximum(ec, 0.0)
        ar, ac = jnp.minimum(dr, 0.0), jnp.minimum(dc, 0.0)
        lap = (dr - er) + (dc - ec)
        ham = 0.5 * ((br * br + ar * ar) + (bc * bc + ac * ac))
        values[t] = u + time_step * (viscosity * lap - ham + own_sum[n])

    stages = [(RELAY, stage_relay), (PARTIAL, stage_partial), (TOTAL, stage_total), (SWEEP, stage_sweep), (STRIP, stage_strip)]
    plan = sorted((first + per * n, k, n) for k, ((first, per), _) in enumerate(stages) for n in range(steps))
    last = plan.index((SWEEP[0] + SWEEP[1] * (steps - 1), 3, steps - 1)) + 1
    for _, k, n in plan[:last]:
        stages[k][1](n)

    sums_n = 1
    sums_all[me] = sums_own[...]
    for z in peers:
        remote(sums_own, sums_all.at[me], back_send.at[sums_n], back_recv.at[sums_n], {"tile": z})

    wait_spread(start_mass, start_recv.at[1])
    u = state["u"]
    mass = start_mass[...].reshape(total_rows, full)
    for t in range(steps):
        if t == 0:
            dr, dc = ahead_r(u) - u, ahead_c(u) - u
        else:
            dr, dc = slope_r[t], slope_c[t]
        mr, mc = ahead_r(mass), ahead_c(mass)
        flux_r = jnp.maximum(-dr, 0.0) * mass + jnp.minimum(-dr, 0.0) * mr
        flux_c = jnp.maximum(-dc, 0.0) * mass + jnp.minimum(-dc, 0.0) * mc
        net_r = viscosity * (mr - mass) - flux_r
        net_c = viscosity * (mc - mass) - flux_c
        mass = mass + time_step * ((net_r - behind_r(net_r)) + (net_c - behind_c(net_c)))
    mass_main[...] = mass[:, :width].reshape(tiles, rows, width)
    send_back(mass_main, density_out, 0)
    for _, k, n in plan[last:]:
        stages[k][1](n)

    arrived(sums_all.at[pl.ds(0, tiles - 1)], back_recv.at[sums_n])
    arrived(sums_all.at[pl.ds(0, tiles - 1)], back_send.at[sums_n])
    grand = jnp.sum(jnp.sum(sums_all[...], axis=0), axis=1, keepdims=True) * (1.0 / (total_rows * cols))
    for t in reversed(range(steps)):
        values[t] = values[t] - grand[t:t + 1, :]
    wait_back(mass_main, density_out, 0)
    wait_spread(start_value, start_send.at[0])
    wait_spread(start_mass, start_send.at[1])
    for g in range(steps // WINDOWS):
        wait_spread(rim_in.at[g], rim_send.at[g])
    for n in range(steps):
        wait_spread(cost_in.at[n], cost_send.at[n])
        wait_spread(edge_in.at[n], edge_send.at[n])
    for copy in sent:
        copy.wait_send()


def finish(values, density, values_out, density_out, sems):
    copies = [
        pltpu.make_async_copy(values, values_out, sems.at[0]),
        pltpu.make_async_copy(density, density_out, sems.at[1]),
    ]
    for copy in copies:
        copy.start()
    for copy in copies:
        copy.wait()


def per_device(pops, tiles, weights, terminal, density_history, density_init):
    _, steps, rows, cols = density_history.shape
    width = cols // tiles
    outer = pops // 4
    total_rows = tiles * rows
    full = width + LANES
    dma = pltpu.SemaphoreType.DMA
    lines = max(outer - 1, 1)
    groups = steps // WINDOWS
    vmem = pl.BlockSpec(memory_space=pltpu.VMEM)
    anywhere = pl.BlockSpec(memory_space=pl.ANY)
    values, density = pl.pallas_call(
        functools.partial(kernel, pops, tiles),
        out_shape=(
            pltpu.VMEM((steps, rows, cols), jnp.float32),
            pltpu.VMEM((rows, cols), jnp.float32),
        ),
        in_specs=[anywhere, anywhere, anywhere, anywhere],
        out_specs=(vmem, vmem),
        scratch_shapes=[
            pltpu.SMEM((pops, pops), jnp.int32),
            pltpu.VMEM((rows, cols), jnp.float32),
            pltpu.VMEM((steps, rows, cols), jnp.bfloat16),
            pltpu.VMEM((rows, cols), jnp.float32),
            dma((4,)),
            pltpu.VMEM((steps, rows, cols), jnp.bfloat16),
            pltpu.VMEM((lines, steps, rows, cols), jnp.bfloat16),
            pltpu.VMEM((lines, steps, rows, cols), jnp.bfloat16),
            pltpu.VMEM((steps, rows, cols), jnp.float32),
            pltpu.VMEM((lines, steps, rows, cols), jnp.int16),
            pltpu.VMEM((lines, steps, rows, cols), jnp.int16),
            pltpu.VMEM((steps, tiles, rows, width), jnp.int16),
            pltpu.VMEM((steps, tiles, rows, width), jnp.int16),
            pltpu.VMEM((groups, tiles, rows, LANES), jnp.int16),
            pltpu.VMEM((groups, tiles, rows, LANES), jnp.int16),
            pltpu.VMEM((tiles, rows, full), jnp.float32),
            pltpu.VMEM((tiles, rows, full), jnp.float32),
            pltpu.VMEM((tiles, rows, full), jnp.float32),
            pltpu.VMEM((tiles, rows, full), jnp.float32),
            pltpu.VMEM((steps, tiles, 2, width), jnp.float32),
            pltpu.VMEM((steps, tiles, 2, width), jnp.float32),
            pltpu.VMEM((tiles, rows, width), jnp.float32),
            pltpu.VMEM((steps, total_rows, full), jnp.float32),
            pltpu.VMEM((steps, total_rows, full), jnp.float32),
            pltpu.VMEM((steps, LANES), jnp.float32),
            pltpu.VMEM((tiles, steps, LANES), jnp.float32),
            dma((steps,)), dma((steps,)),
            dma((lines, steps)), dma((lines, steps)),
            dma((lines, steps)), dma((lines, steps)),
            dma((lines, steps)), dma((lines, steps)),
            dma((steps,)), dma((steps,)),
            dma((groups,)), dma((groups,)),
            dma((2,)), dma((2,)),
            dma((steps,)), dma((steps,)),
            dma((2,)), dma((2,)), dma((1,)),
        ],
        compiler_params=pltpu.CompilerParams(collective_id=0, has_side_effects=True),
    )(weights, terminal[0], density_history[0], density_init[0])
    values, density = pl.pallas_call(
        finish,
        out_shape=(
            jax.ShapeDtypeStruct((steps, rows, cols), jnp.float32),
            jax.ShapeDtypeStruct((rows, cols), jnp.float32),
        ),
        in_specs=[anywhere, anywhere],
        out_specs=(anywhere, anywhere),
        scratch_shapes=[dma((2,))],
        compiler_params=pltpu.CompilerParams(vmem_limit_bytes=8 * 1024 * 1024),
    )(values, density)
    return values[None], density[None]


def solution(mesh):
    in_specs = (P(), P("pop", "tile", None), P("pop", None, "tile", None), P("pop", "tile", None))
    out_specs = (P("pop", None, "tile", None), P("pop", "tile", None))
    body = functools.partial(per_device, mesh.shape["pop"], mesh.shape["tile"])
    return jax.shard_map(body, mesh=mesh, in_specs=in_specs, out_specs=out_specs, check_vma=False)
```

```python
import functools

import jax
import jax.numpy as jnp
from jax import lax
from jax.experimental import pallas as pl
from jax.experimental.pallas import tpu as pltpu
from jax.sharding import PartitionSpec as P

time_step = 0.2
viscosity = 0.2
LANES = 128
WINDOWS = 4
SPAN = LANES // WINDOWS
CHUNK = 512
CENTRE = 1.1
LARGEST = 3.0 * 0.901
LEVELS = 32400.0
RELAY = (2.6, 0.35)
PARTIAL = (3.6, 0.35)
TOTAL = (6.4, 0.6)
SWEEP = (12.5, 0.9)
STRIP = (20.0, 0.65)


def kernel(pops, tiles, weights_in, terminal_in, history_in, initial_in, values, density_out,
           weights, terminal, history, initial, load_sem, near_other, near, near_relay, own_sum, part_out, part_in,
           cost_out, cost_in, rim_out, rim_in, value_out, start_value, mass_out, start_mass, edge_out, edge_in, mass_main, slope_r, slope_c, sums_own, sums_all,
           other_send, other_recv, near_send, near_recv, relay_send, relay_recv, part_send, part_recv,
           cost_send, cost_recv, rim_send, rim_recv, start_send, start_recv,
           edge_send, edge_recv, back_send, back_recv, back_self):
    steps, rows, cols = history.shape
    width = cols // tiles
    full = width + LANES
    total_rows = tiles * rows
    outer = pops // 4
    me = lax.axis_index("tile")
    own = lax.axis_index("pop")
    core = own % 2
    plane = (own // 2) % 2
    line = own // 4

    def pop_of(a, b, c):
        return (a * 2 + b) * 2 + c

    partner = pop_of(line, plane, 1 - core)
    across = pop_of(line, 1 - plane, core)
    columns = [pop_of((line + j) % outer, plane, core) for j in range(1, outer)]
    behind = [(line + outer - j) % outer for j in range(1, outer)]

    def along_row(n):
        return n % 2 == 0 or outer == 1

    def first_peers(n):
        return [across] if along_row(n) else columns

    def second_peers(n):
        return columns if along_row(n) else [across]

    def sources(n):
        far = [(line, 1 - plane)] if along_row(n) else [(a, plane) for a in behind]
        return [own, partner] + [pop_of(a, b, core) for a, b in far] + [pop_of(a, b, 1 - core) for a, b in far]

    peers = [(me + d) % tiles for d in range(1, tiles)]

    barrier = pltpu.get_barrier_semaphore()
    greeted = [{"tile": z} for z in peers] + [{"pop": q} for q in [partner, across] + columns]
    for there in greeted:
        pl.semaphore_signal(barrier, inc=1, device_id=there, device_id_type=pl.DeviceIdType.MESH)

    loads = [pltpu.make_async_copy(src, dst, load_sem.at[n]) for n, (src, dst) in enumerate(
        [(weights_in, weights), (terminal_in, terminal), (initial_in, initial), (history_in, history)])]
    for load in loads:
        load.start()
    for load in loads:
        load.wait()
    lane = lax.broadcasted_iota(jnp.int32, (rows, LANES), 1)
    window = ((lane + SPAN // 2) % LANES) // SPAN
    right_side = lax.broadcasted_iota(jnp.int32, (rows, LANES), 1) < LANES // 2

    def main_of(block, z):
        return block[:, z * width:(z + 1) * width]

    def rim_of(block, z):
        right = ((z + 1) % tiles) * width
        left = ((z + tiles - 1) % tiles) * width + width - LANES
        return jnp.where(right_side, block[:, right:right + LANES], block[:, left:left + LANES])

    for src, dst in [(terminal, value_out), (initial, mass_out)]:
        block = src[...]
        for z in range(tiles):
            dst[z, :, :width] = main_of(block, z)
            dst[z, :, width:] = rim_of(block, z)
    start_value[me] = value_out[me]
    start_mass[me] = mass_out[me]

    pl.semaphore_wait(barrier, len(greeted))

    def cut(z):
        return pl.ds(pl.multiple_of(z * width, LANES), width)

    sent = []

    def remote(src, dst, send, recv, there):
        copy = pltpu.make_async_remote_copy(src_ref=src, dst_ref=dst, send_sem=send, recv_sem=recv,
                                            device_id=there, device_id_type=pl.DeviceIdType.MESH)
        copy.start()
        return copy

    def arrived(ref, sem):
        pltpu.make_async_copy(ref, ref, sem).wait()

    def spread(src, dst, send, recv):
        for z in peers:
            remote(src.at[z], dst.at[me], send, recv, {"tile": z})

    def wait_spread(dst, sem):
        arrived(dst.at[pl.ds(0, tiles - 1)], sem)

    for n in range(steps):
        t = steps - 1 - n
        for j, q in enumerate(first_peers(n)):
            sent.append(remote(history.at[t], near.at[j, t], near_send.at[j, n], near_recv.at[j, n], {"pop": q}))
        sent.append(remote(history.at[t], near_other.at[t], other_send.at[n], other_recv.at[n], {"pop": partner}))
    spread(value_out, start_value, start_send.at[0], start_recv.at[0])
    spread(mass_out, start_mass, start_send.at[1], start_recv.at[1])

    def weight(p, q):
        return weights[p, q].astype(jnp.float32) * (1.0 / pops)

    def part_step(n):
        return LARGEST * (4.0 if along_row(n) else 2.0 * outer) / pops / LEVELS

    cost_step = LARGEST / LEVELS

    def coded(x, step):
        return jnp.round(x * (1.0 / step)).astype(jnp.int32).astype(jnp.int16)

    def decoded(x, step):
        return x.astype(jnp.int32).astype(jnp.float32) * step

    def stage_relay(n):
        t = steps - 1 - n
        for j in range(len(first_peers(n))):
            arrived(near.at[j, t], near_recv.at[j, n])
            sent.append(remote(near.at[j, t], near_relay.at[j, t], relay_send.at[j, n], relay_recv.at[j, n],
                               {"pop": partner}))

    def stage_partial(n):
        t = steps - 1 - n
        far = range(len(first_peers(n)))
        arrived(near_other.at[t], other_recv.at[n])
        for j in far:
            arrived(near_relay.at[j, t], relay_recv.at[j, n])
        own_factors = [weight(own, q) for q in sources(n)]
        part_factors = [[weight(p, q) for q in sources(n)] for p in second_peers(n)]
        for c in range(0, cols, CHUNK):
            span = slice(c, c + CHUNK)
            blocks = [history[t, :, span], near_other[t, :, span]]
            blocks += [near[j, t, :, span] for j in far] + [near_relay[j, t, :, span] for j in far]
            blocks = [b.astype(jnp.float32) - CENTRE for b in blocks]

            def mixed(factors):
                total = factors[0] * blocks[0]
                for f, b in zip(factors[1:], blocks[1:]):
                    total = total + f * b
                return total

            for j, factors in enumerate(part_factors):
                part_out[j, n, :, span] = coded(mixed(factors), part_step(n))
            own_sum[n, :, span] = mixed(own_factors)
        for j, q in enumerate(second_peers(n)):
            sent.append(remote(part_out.at[j, n], part_in.at[j, n], part_send.at[j, n], part_recv.at[j, n], {"pop": q}))

    def stage_total(n):
        if n == 0:
            wait_spread(start_value, start_recv.at[0])
            send_edges(start_value[:, :, :width].reshape(total_rows, width), 0)
        total = own_sum[n]
        for j in range(len(second_peers(n))):
            arrived(part_in.at[j, n], part_recv.at[j, n])
            total = total + decoded(part_in[j, n], part_step(n))
        own_sum[n] = total
        for z in range(tiles):
            cost_out[n, z] = coded(main_of(total, z), cost_step)
        spread(cost_out.at[n], cost_in.at[n], cost_send.at[n], cost_recv.at[n])
        cost_in[n, me] = cost_out[n, me]
        g, k = n // WINDOWS, n % WINDOWS
        if k == WINDOWS - 1:
            for z in range(tiles):
                rim = rim_of(own_sum[g * WINDOWS], z)
                for i in range(1, WINDOWS):
                    rim = jnp.where(window == i, pltpu.roll(rim_of(own_sum[g * WINDOWS + i], z), SPAN * i, 1), rim)
                rim_out[g, z] = coded(rim, cost_step)
            spread(rim_out.at[g], rim_in.at[g], rim_send.at[g], rim_recv.at[g])
            rim_in[g, me] = rim_out[g, me]

    def ahead_r(x):
        return pltpu.roll(x, total_rows - 1, 0)

    def behind_r(x):
        return pltpu.roll(x, 1, 0)

    def ahead_c(x):
        return pltpu.roll(x, full - 1, 1)

    def behind_c(x):
        return pltpu.roll(x, 1, 1)

    def send_edges(main, n):
        for z in range(tiles):
            above = (z * rows + total_rows - 1) % total_rows
            below = (z * rows + rows) % total_rows
            edge_out[n, z, 0:1, :] = main[above:above + 1, :]
            edge_out[n, z, 1:2, :] = main[below:below + 1, :]
        spread(edge_out.at[n], edge_in.at[n], edge_send.at[n], edge_recv.at[n])
        edge_in[n, me] = edge_out[n, me]

    def send_back(src, dst, n):
        pltpu.make_async_copy(src.at[me], dst.at[:, cut(me)], back_self.at[n]).start()
        for z in peers:
            remote(src.at[z], dst.at[:, cut(me)], back_send.at[n], back_recv.at[n], {"tile": z})

    def wait_back(src, dst, n):
        pltpu.make_async_copy(src.at[me], dst.at[:, cut(me)], back_self.at[n]).wait()
        landed = dst.at[:, pl.ds(0, (tiles - 1) * width)]
        arrived(landed, back_recv.at[n])
        arrived(landed, back_send.at[n])

    state = {}

    def stage_sweep(n):
        t = steps - 1 - n
        if n == 0:
            state["u"] = start_value[...].reshape(total_rows, full)
        wait_spread(cost_in.at[n], cost_recv.at[n])
        g, k = n // WINDOWS, n % WINDOWS
        if k == 0:
            wait_spread(rim_in.at[g], rim_recv.at[g])
            state["rim"] = decoded(rim_in[g], cost_step).reshape(total_rows, LANES)
        rim = state["rim"] if k == 0 else pltpu.roll(state["rim"], LANES - SPAN * k, 1)
        source = jnp.concatenate([decoded(cost_in[n], cost_step).reshape(total_rows, width), rim], axis=1)
        u = state["u"]
        dr = ahead_r(u) - u
        dc = ahead_c(u) - u
        if t + 1 < steps:
            slope_r[t + 1] = dr
            slope_c[t + 1] = dc
        er, ec = behind_r(dr), behind_c(dc)
        br, bc = jnp.maximum(er, 0.0), jnp.maximum(ec, 0.0)
        ar, ac = jnp.minimum(dr, 0.0), jnp.minimum(dc, 0.0)
        lap = (dr - er) + (dc - ec)
        ham = 0.5 * ((br * br + ar * ar) + (bc * bc + ac * ac))
        u = u + time_step * (viscosity * lap - ham + source)
        state["u"] = u
        main = u[:, :width]
        if t > 0:
            send_edges(main, n + 1)
        line_sum = jnp.sum(main, axis=0, keepdims=True)
        folded = line_sum[:, :LANES]
        for j in range(1, width // LANES):
            folded = folded + line_sum[:, j * LANES:(j + 1) * LANES]
        sums_own[t:t + 1, :] = folded

    row = lax.broadcasted_iota(jnp.int32, (rows, cols), 0)

    def stage_strip(n):
        t = steps - 1 - n
        wait_spread(edge_in.at[n], edge_recv.at[n])
        above = jnp.concatenate([edge_in[n, z, 0:1, :] for z in range(tiles)], axis=1)
        below = jnp.concatenate([edge_in[n, z, 1:2, :] for z in range(tiles)], axis=1)
        u = terminal[...] if n == 0 else values[t + 1]
        dr = jnp.where(row == rows - 1, below, pltpu.roll(u, rows - 1, 0)) - u
        er = u - jnp.where(row == 0, above, pltpu.roll(u, 1, 0))
        dc = pltpu.roll(u, cols - 1, 1) - u
        ec = pltpu.roll(dc, 1, 1)
        br, bc = jnp.maximum(er, 0.0), jnp.maximum(ec, 0.0)
        ar, ac = jnp.minimum(dr, 0.0), jnp.minimum(dc, 0.0)
        lap = (dr - er) + (dc - ec)
        ham = 0.5 * ((br * br + ar * ar) + (bc * bc + ac * ac))
        values[t] = u + time_step * (viscosity * lap - ham + own_sum[n])

    stages = [(RELAY, stage_relay), (PARTIAL, stage_partial), (TOTAL, stage_total), (SWEEP, stage_sweep), (STRIP, stage_strip)]
    plan = sorted((first + per * n, k, n) for k, ((first, per), _) in enumerate(stages) for n in range(steps))
    last = plan.index((SWEEP[0] + SWEEP[1] * (steps - 1), 3, steps - 1)) + 1
    for _, k, n in plan[:last]:
        stages[k][1](n)

    sums_n = 1
    sums_all[me] = sums_own[...]
    for z in peers:
        remote(sums_own, sums_all.at[me], back_send.at[sums_n], back_recv.at[sums_n], {"tile": z})

    wait_spread(start_mass, start_recv.at[1])
    u = state["u"]
    mass = start_mass[...].reshape(total_rows, full)
    for t in range(steps):
        if t == 0:
            dr, dc = ahead_r(u) - u, ahead_c(u) - u
        else:
            dr, dc = slope_r[t], slope_c[t]
        pr, qr = viscosity + jnp.maximum(dr, 0.0), viscosity + jnp.maximum(-dr, 0.0)
        pc, qc = viscosity + jnp.maximum(dc, 0.0), viscosity + jnp.maximum(-dc, 0.0)
        ec = behind_c(dc)
        bc, kc = viscosity + jnp.maximum(ec, 0.0), viscosity + jnp.maximum(-ec, 0.0)
        net_r = pr * ahead_r(mass) - qr * mass
        net_c = (pc * ahead_c(mass) - qc * mass) - (bc * mass - kc * behind_c(mass))
        mass = mass + time_step * ((net_r - behind_r(net_r)) + net_c)
    mass_main[...] = mass[:, :width].reshape(tiles, rows, width)
    send_back(mass_main, density_out, 0)
    for _, k, n in plan[last:]:
        stages[k][1](n)

    arrived(sums_all.at[pl.ds(0, tiles - 1)], back_recv.at[sums_n])
    arrived(sums_all.at[pl.ds(0, tiles - 1)], back_send.at[sums_n])
    grand = jnp.sum(jnp.sum(sums_all[...], axis=0), axis=1, keepdims=True) * (1.0 / (total_rows * cols))
    for t in reversed(range(steps)):
        values[t] = values[t] - grand[t:t + 1, :]
    wait_back(mass_main, density_out, 0)
    wait_spread(start_value, start_send.at[0])
    wait_spread(start_mass, start_send.at[1])
    for g in range(steps // WINDOWS):
        wait_spread(rim_in.at[g], rim_send.at[g])
    for n in range(steps):
        wait_spread(cost_in.at[n], cost_send.at[n])
        wait_spread(edge_in.at[n], edge_send.at[n])
    for copy in sent:
        copy.wait_send()


def finish(values, density, values_out, density_out, sems):
    copies = [
        pltpu.make_async_copy(values, values_out, sems.at[0]),
        pltpu.make_async_copy(density, density_out, sems.at[1]),
    ]
    for copy in copies:
        copy.start()
    for copy in copies:
        copy.wait()


def per_device(pops, tiles, weights, terminal, density_history, density_init):
    _, steps, rows, cols = density_history.shape
    width = cols // tiles
    outer = pops // 4
    total_rows = tiles * rows
    full = width + LANES
    dma = pltpu.SemaphoreType.DMA
    lines = max(outer - 1, 1)
    groups = steps // WINDOWS
    vmem = pl.BlockSpec(memory_space=pltpu.VMEM)
    anywhere = pl.BlockSpec(memory_space=pl.ANY)
    values, density = pl.pallas_call(
        functools.partial(kernel, pops, tiles),
        out_shape=(
            pltpu.VMEM((steps, rows, cols), jnp.float32),
            pltpu.VMEM((rows, cols), jnp.float32),
        ),
        in_specs=[anywhere, anywhere, anywhere, anywhere],
        out_specs=(vmem, vmem),
        scratch_shapes=[
            pltpu.SMEM((pops, pops), jnp.int32),
            pltpu.VMEM((rows, cols), jnp.float32),
            pltpu.VMEM((steps, rows, cols), jnp.bfloat16),
            pltpu.VMEM((rows, cols), jnp.float32),
            dma((4,)),
            pltpu.VMEM((steps, rows, cols), jnp.bfloat16),
            pltpu.VMEM((lines, steps, rows, cols), jnp.bfloat16),
            pltpu.VMEM((lines, steps, rows, cols), jnp.bfloat16),
            pltpu.VMEM((steps, rows, cols), jnp.float32),
            pltpu.VMEM((lines, steps, rows, cols), jnp.int16),
            pltpu.VMEM((lines, steps, rows, cols), jnp.int16),
            pltpu.VMEM((steps, tiles, rows, width), jnp.int16),
            pltpu.VMEM((steps, tiles, rows, width), jnp.int16),
            pltpu.VMEM((groups, tiles, rows, LANES), jnp.int16),
            pltpu.VMEM((groups, tiles, rows, LANES), jnp.int16),
            pltpu.VMEM((tiles, rows, full), jnp.float32),
            pltpu.VMEM((tiles, rows, full), jnp.float32),
            pltpu.VMEM((tiles, rows, full), jnp.float32),
            pltpu.VMEM((tiles, rows, full), jnp.float32),
            pltpu.VMEM((steps, tiles, 2, width), jnp.float32),
            pltpu.VMEM((steps, tiles, 2, width), jnp.float32),
            pltpu.VMEM((tiles, rows, width), jnp.float32),
            pltpu.VMEM((steps, total_rows, full), jnp.float32),
            pltpu.VMEM((steps, total_rows, full), jnp.float32),
            pltpu.VMEM((steps, LANES), jnp.float32),
            pltpu.VMEM((tiles, steps, LANES), jnp.float32),
            dma((steps,)), dma((steps,)),
            dma((lines, steps)), dma((lines, steps)),
            dma((lines, steps)), dma((lines, steps)),
            dma((lines, steps)), dma((lines, steps)),
            dma((steps,)), dma((steps,)),
            dma((groups,)), dma((groups,)),
            dma((2,)), dma((2,)),
            dma((steps,)), dma((steps,)),
            dma((2,)), dma((2,)), dma((1,)),
        ],
        compiler_params=pltpu.CompilerParams(collective_id=0, has_side_effects=True),
    )(weights, terminal[0], density_history[0], density_init[0])
    values, density = pl.pallas_call(
        finish,
        out_shape=(
            jax.ShapeDtypeStruct((steps, rows, cols), jnp.float32),
            jax.ShapeDtypeStruct((rows, cols), jnp.float32),
        ),
        in_specs=[anywhere, anywhere],
        out_specs=(anywhere, anywhere),
        scratch_shapes=[dma((2,))],
        compiler_params=pltpu.CompilerParams(vmem_limit_bytes=8 * 1024 * 1024),
    )(values, density)
    return values[None], density[None]


def solution(mesh):
    in_specs = (P(), P("pop", "tile", None), P("pop", None, "tile", None), P("pop", "tile", None))
    out_specs = (P("pop", None, "tile", None), P("pop", "tile", None))
    body = functools.partial(per_device, mesh.shape["pop"], mesh.shape["tile"])
    return jax.shard_map(body, mesh=mesh, in_specs=in_specs, out_specs=out_specs, check_vma=False)
```

```python
import functools

import jax
import jax.numpy as jnp
from jax import lax
from jax.experimental import pallas as pl
from jax.experimental.pallas import tpu as pltpu
from jax.sharding import PartitionSpec as P

time_step = 0.2
viscosity = 0.2
LANES = 128
WINDOWS = 4
SPAN = LANES // WINDOWS
CHUNK = 512
BOTH = (0, 1)
CENTRE = 1.1
LARGEST = 3.0 * 0.901
LEVELS = 32400.0
RELAY = (2.6, 0.35)
PARTIAL = (3.6, 0.35)
TOTAL = (6.4, 0.6)
SWEEP = (12.5, 0.9)
STRIP = (20.0, 0.65)


def kernel(pops, tiles, weights_in, terminal_in, history_in, initial_in, values, density_out,
           weights, terminal, history, initial, load_sem, near_other, near, near_relay, own_sum, part_out, part_in,
           cost_out, cost_in, rim_out, rim_in, value_out, start_value, mass_out, start_mass, edge_out, edge_in, mass_main, slope_r, slope_c, sums_own, sums_all,
           other_send, other_recv, near_send, near_recv, relay_send, relay_recv, part_send, part_recv,
           cost_send, cost_recv, rim_send, rim_recv, start_send, start_recv,
           edge_send, edge_recv, back_send, back_recv, back_self):
    steps, rows, cols = history.shape
    width = cols // tiles
    full = width + LANES
    total_rows = tiles * rows
    outer = pops // 4
    me = lax.axis_index("tile")
    own = lax.axis_index("pop")
    core = own % 2
    plane = (own // 2) % 2
    line = own // 4

    def pop_of(a, b, c):
        return (a * 2 + b) * 2 + c

    partner = pop_of(line, plane, 1 - core)
    across = pop_of(line, 1 - plane, core)
    columns = [pop_of((line + j) % outer, plane, core) for j in range(1, outer)]
    behind = [(line + outer - j) % outer for j in range(1, outer)]

    def along_row(n):
        return n % 2 == 0 or outer == 1

    def first_peers(n):
        return [across] if along_row(n) else columns

    def flipped(q):
        return q + 1 - 2 * (q % 2)

    def second_peers(n):
        return columns if along_row(n) else [across]

    def sources(n):
        far = [(line, 1 - plane)] if along_row(n) else [(a, plane) for a in behind]
        return [own, partner] + [pop_of(a, b, core) for a, b in far] + [pop_of(a, b, 1 - core) for a, b in far]

    peers = [(me + d) % tiles for d in range(1, tiles)]

    barrier = pltpu.get_barrier_semaphore()
    greeted = [{"tile": z} for z in peers] + [{"pop": q} for q in [partner, across] + columns + [flipped(q) for q in [across] + columns]]
    for there in greeted:
        pl.semaphore_signal(barrier, inc=1, device_id=there, device_id_type=pl.DeviceIdType.MESH)

    loads = [pltpu.make_async_copy(src, dst, load_sem.at[n]) for n, (src, dst) in enumerate(
        [(weights_in, weights), (terminal_in, terminal), (initial_in, initial), (history_in, history)])]
    for load in loads:
        load.start()
    for load in loads:
        load.wait()
    lane = lax.broadcasted_iota(jnp.int32, (rows, LANES), 1)
    window = ((lane + SPAN // 2) % LANES) // SPAN
    right_side = lax.broadcasted_iota(jnp.int32, (rows, LANES), 1) < LANES // 2

    def main_of(block, z):
        return block[:, z * width:(z + 1) * width]

    def rim_of(block, z):
        right = ((z + 1) % tiles) * width
        left = ((z + tiles - 1) % tiles) * width + width - LANES
        return jnp.where(right_side, block[:, right:right + LANES], block[:, left:left + LANES])

    for src, dst in [(terminal, value_out), (initial, mass_out)]:
        block = src[...]
        for z in range(tiles):
            dst[z, :, :width] = main_of(block, z)
            dst[z, :, width:] = rim_of(block, z)
    start_value[me] = value_out[me]
    start_mass[me] = mass_out[me]

    pl.semaphore_wait(barrier, len(greeted))

    def cut(z):
        return pl.ds(pl.multiple_of(z * width, LANES), width)

    sent = []

    def remote(src, dst, send, recv, there):
        copy = pltpu.make_async_remote_copy(src_ref=src, dst_ref=dst, send_sem=send, recv_sem=recv,
                                            device_id=there, device_id_type=pl.DeviceIdType.MESH)
        copy.start()
        return copy

    def arrived(ref, sem):
        pltpu.make_async_copy(ref, ref, sem).wait()

    def spread(src, dst, send, recv):
        for z in peers:
            remote(src.at[z], dst.at[me], send, recv, {"tile": z})

    def wait_spread(dst, sem):
        arrived(dst.at[pl.ds(0, tiles - 1)], sem)

    for n in range(steps):
        t = steps - 1 - n
        for j, q in enumerate(first_peers(n)):
            sent.append(remote(history.at[t], near.at[j, t], near_send.at[j, n], near_recv.at[j, n], {"pop": q}))
            if n in BOTH:
                sent.append(remote(history.at[t], near_relay.at[j, t], relay_send.at[j, n], relay_recv.at[j, n],
                                   {"pop": flipped(q)}))
        sent.append(remote(history.at[t], near_other.at[t], other_send.at[n], other_recv.at[n], {"pop": partner}))
    spread(value_out, start_value, start_send.at[0], start_recv.at[0])
    spread(mass_out, start_mass, start_send.at[1], start_recv.at[1])

    def weight(p, q):
        return weights[p, q].astype(jnp.float32) * (1.0 / pops)

    def part_step(n):
        return LARGEST * (4.0 if along_row(n) else 2.0 * outer) / pops / LEVELS

    cost_step = LARGEST / LEVELS

    def coded(x, step):
        return jnp.round(x * (1.0 / step)).astype(jnp.int32).astype(jnp.int16)

    def decoded(x, step):
        return x.astype(jnp.int32).astype(jnp.float32) * step

    def stage_relay(n):
        t = steps - 1 - n
        for j in range(len(first_peers(n))):
            arrived(near.at[j, t], near_recv.at[j, n])
            if n in BOTH:
                continue
            sent.append(remote(near.at[j, t], near_relay.at[j, t], relay_send.at[j, n], relay_recv.at[j, n],
                               {"pop": partner}))

    def stage_partial(n):
        t = steps - 1 - n
        far = range(len(first_peers(n)))
        arrived(near_other.at[t], other_recv.at[n])
        for j in far:
            arrived(near_relay.at[j, t], relay_recv.at[j, n])
        own_factors = [weight(own, q) for q in sources(n)]
        part_factors = [[weight(p, q) for q in sources(n)] for p in second_peers(n)]
        for c in range(0, cols, CHUNK):
            span = slice(c, c + CHUNK)
            blocks = [history[t, :, span], near_other[t, :, span]]
            blocks += [near[j, t, :, span] for j in far] + [near_relay[j, t, :, span] for j in far]
            blocks = [b.astype(jnp.float32) - CENTRE for b in blocks]

            def mixed(factors):
                total = factors[0] * blocks[0]
                for f, b in zip(factors[1:], blocks[1:]):
                    total = total + f * b
                return total

            for j, factors in enumerate(part_factors):
                part_out[j, n, :, span] = coded(mixed(factors), part_step(n))
            own_sum[n, :, span] = mixed(own_factors)
        for j, q in enumerate(second_peers(n)):
            sent.append(remote(part_out.at[j, n], part_in.at[j, n], part_send.at[j, n], part_recv.at[j, n], {"pop": q}))

    def stage_total(n):
        if n == 0:
            wait_spread(start_value, start_recv.at[0])
            send_edges(start_value[:, :, :width].reshape(total_rows, width), 0)
        total = own_sum[n]
        for j in range(len(second_peers(n))):
            arrived(part_in.at[j, n], part_recv.at[j, n])
            total = total + decoded(part_in[j, n], part_step(n))
        own_sum[n] = total
        for z in range(tiles):
            cost_out[n, z] = coded(main_of(total, z), cost_step)
        spread(cost_out.at[n], cost_in.at[n], cost_send.at[n], cost_recv.at[n])
        cost_in[n, me] = cost_out[n, me]
        g, k = n // WINDOWS, n % WINDOWS
        if k == WINDOWS - 1:
            for z in range(tiles):
                rim = rim_of(own_sum[g * WINDOWS], z)
                for i in range(1, WINDOWS):
                    rim = jnp.where(window == i, pltpu.roll(rim_of(own_sum[g * WINDOWS + i], z), SPAN * i, 1), rim)
                rim_out[g, z] = coded(rim, cost_step)
            spread(rim_out.at[g], rim_in.at[g], rim_send.at[g], rim_recv.at[g])
            rim_in[g, me] = rim_out[g, me]

    def ahead_r(x):
        return pltpu.roll(x, total_rows - 1, 0)

    def behind_r(x):
        return pltpu.roll(x, 1, 0)

    def ahead_c(x):
        return pltpu.roll(x, full - 1, 1)

    def behind_c(x):
        return pltpu.roll(x, 1, 1)

    def send_edges(main, n):
        for z in range(tiles):
            above = (z * rows + total_rows - 1) % total_rows
            below = (z * rows + rows) % total_rows
            edge_out[n, z, 0:1, :] = main[above:above + 1, :]
            edge_out[n, z, 1:2, :] = main[below:below + 1, :]
        spread(edge_out.at[n], edge_in.at[n], edge_send.at[n], edge_recv.at[n])
        edge_in[n, me] = edge_out[n, me]

    def send_back(src, dst, n):
        pltpu.make_async_copy(src.at[me], dst.at[:, cut(me)], back_self.at[n]).start()
        for z in peers:
            remote(src.at[z], dst.at[:, cut(me)], back_send.at[n], back_recv.at[n], {"tile": z})

    def wait_back(src, dst, n):
        pltpu.make_async_copy(src.at[me], dst.at[:, cut(me)], back_self.at[n]).wait()
        landed = dst.at[:, pl.ds(0, (tiles - 1) * width)]
        arrived(landed, back_recv.at[n])
        arrived(landed, back_send.at[n])

    state = {}

    def stage_sweep(n):
        t = steps - 1 - n
        if n == 0:
            state["u"] = start_value[...].reshape(total_rows, full)
        wait_spread(cost_in.at[n], cost_recv.at[n])
        g, k = n // WINDOWS, n % WINDOWS
        if k == 0:
            wait_spread(rim_in.at[g], rim_recv.at[g])
            state["rim"] = decoded(rim_in[g], cost_step).reshape(total_rows, LANES)
        rim = state["rim"] if k == 0 else pltpu.roll(state["rim"], LANES - SPAN * k, 1)
        source = jnp.concatenate([decoded(cost_in[n], cost_step).reshape(total_rows, width), rim], axis=1)
        u = state["u"]
        dr = ahead_r(u) - u
        dc = ahead_c(u) - u
        if t + 1 < steps:
            slope_r[t + 1] = dr
            slope_c[t + 1] = dc
        er, ec = behind_r(dr), behind_c(dc)
        br, bc = jnp.maximum(er, 0.0), jnp.maximum(ec, 0.0)
        ar, ac = jnp.minimum(dr, 0.0), jnp.minimum(dc, 0.0)
        lap = (dr - er) + (dc - ec)
        ham = 0.5 * ((br * br + ar * ar) + (bc * bc + ac * ac))
        u = u + time_step * (viscosity * lap - ham + source)
        state["u"] = u
        main = u[:, :width]
        if t > 0:
            send_edges(main, n + 1)
        line_sum = jnp.sum(main, axis=0, keepdims=True)
        folded = line_sum[:, :LANES]
        for j in range(1, width // LANES):
            folded = folded + line_sum[:, j * LANES:(j + 1) * LANES]
        sums_own[t:t + 1, :] = folded

    row = lax.broadcasted_iota(jnp.int32, (rows, cols), 0)

    def stage_strip(n):
        t = steps - 1 - n
        wait_spread(edge_in.at[n], edge_recv.at[n])
        above = jnp.concatenate([edge_in[n, z, 0:1, :] for z in range(tiles)], axis=1)
        below = jnp.concatenate([edge_in[n, z, 1:2, :] for z in range(tiles)], axis=1)
        u = terminal[...] if n == 0 else values[t + 1]
        dr = jnp.where(row == rows - 1, below, pltpu.roll(u, rows - 1, 0)) - u
        er = u - jnp.where(row == 0, above, pltpu.roll(u, 1, 0))
        dc = pltpu.roll(u, cols - 1, 1) - u
        ec = pltpu.roll(dc, 1, 1)
        br, bc = jnp.maximum(er, 0.0), jnp.maximum(ec, 0.0)
        ar, ac = jnp.minimum(dr, 0.0), jnp.minimum(dc, 0.0)
        lap = (dr - er) + (dc - ec)
        ham = 0.5 * ((br * br + ar * ar) + (bc * bc + ac * ac))
        values[t] = u + time_step * (viscosity * lap - ham + own_sum[n])

    stages = [(RELAY, stage_relay), (PARTIAL, stage_partial), (TOTAL, stage_total), (SWEEP, stage_sweep), (STRIP, stage_strip)]
    plan = sorted((first + per * n, k, n) for k, ((first, per), _) in enumerate(stages) for n in range(steps))
    last = plan.index((SWEEP[0] + SWEEP[1] * (steps - 1), 3, steps - 1)) + 1
    for _, k, n in plan[:last]:
        stages[k][1](n)

    sums_n = 1
    sums_all[me] = sums_own[...]
    for z in peers:
        remote(sums_own, sums_all.at[me], back_send.at[sums_n], back_recv.at[sums_n], {"tile": z})

    wait_spread(start_mass, start_recv.at[1])
    u = state["u"]
    mass = start_mass[...].reshape(total_rows, full)
    for t in range(steps):
        if t == 0:
            dr, dc = ahead_r(u) - u, ahead_c(u) - u
        else:
            dr, dc = slope_r[t], slope_c[t]
        pr, qr = viscosity + jnp.maximum(dr, 0.0), viscosity + jnp.maximum(-dr, 0.0)
        pc, qc = viscosity + jnp.maximum(dc, 0.0), viscosity + jnp.maximum(-dc, 0.0)
        ec = behind_c(dc)
        bc, kc = viscosity + jnp.maximum(ec, 0.0), viscosity + jnp.maximum(-ec, 0.0)
        net_r = pr * ahead_r(mass) - qr * mass
        net_c = (pc * ahead_c(mass) - qc * mass) - (bc * mass - kc * behind_c(mass))
        mass = mass + time_step * ((net_r - behind_r(net_r)) + net_c)
    mass_main[...] = mass[:, :width].reshape(tiles, rows, width)
    send_back(mass_main, density_out, 0)
    wait_spread(start_value, start_send.at[0])
    wait_spread(start_mass, start_send.at[1])
    for g in range(steps // WINDOWS):
        wait_spread(rim_in.at[g], rim_send.at[g])
    for n in range(steps):
        wait_spread(cost_in.at[n], cost_send.at[n])
    for copy in sent:
        copy.wait_send()
    for _, k, n in plan[last:]:
        stages[k][1](n)

    arrived(sums_all.at[pl.ds(0, tiles - 1)], back_recv.at[sums_n])
    arrived(sums_all.at[pl.ds(0, tiles - 1)], back_send.at[sums_n])
    grand = jnp.sum(jnp.sum(sums_all[...], axis=0), axis=1, keepdims=True) * (1.0 / (total_rows * cols))
    for t in reversed(range(steps)):
        values[t] = values[t] - grand[t:t + 1, :]
    wait_back(mass_main, density_out, 0)
    for n in range(steps):
        wait_spread(edge_in.at[n], edge_send.at[n])


def finish(values, density, values_out, density_out, sems):
    copies = [
        pltpu.make_async_copy(values, values_out, sems.at[0]),
        pltpu.make_async_copy(density, density_out, sems.at[1]),
    ]
    for copy in copies:
        copy.start()
    for copy in copies:
        copy.wait()


def per_device(pops, tiles, weights, terminal, density_history, density_init):
    _, steps, rows, cols = density_history.shape
    width = cols // tiles
    outer = pops // 4
    total_rows = tiles * rows
    full = width + LANES
    dma = pltpu.SemaphoreType.DMA
    lines = max(outer - 1, 1)
    groups = steps // WINDOWS
    vmem = pl.BlockSpec(memory_space=pltpu.VMEM)
    anywhere = pl.BlockSpec(memory_space=pl.ANY)
    values, density = pl.pallas_call(
        functools.partial(kernel, pops, tiles),
        out_shape=(
            pltpu.VMEM((steps, rows, cols), jnp.float32),
            pltpu.VMEM((rows, cols), jnp.float32),
        ),
        in_specs=[anywhere, anywhere, anywhere, anywhere],
        out_specs=(vmem, vmem),
        scratch_shapes=[
            pltpu.SMEM((pops, pops), jnp.int32),
            pltpu.VMEM((rows, cols), jnp.float32),
            pltpu.VMEM((steps, rows, cols), jnp.bfloat16),
            pltpu.VMEM((rows, cols), jnp.float32),
            dma((4,)),
            pltpu.VMEM((steps, rows, cols), jnp.bfloat16),
            pltpu.VMEM((lines, steps, rows, cols), jnp.bfloat16),
            pltpu.VMEM((lines, steps, rows, cols), jnp.bfloat16),
            pltpu.VMEM((steps, rows, cols), jnp.float32),
            pltpu.VMEM((lines, steps, rows, cols), jnp.int16),
            pltpu.VMEM((lines, steps, rows, cols), jnp.int16),
            pltpu.VMEM((steps, tiles, rows, width), jnp.int16),
            pltpu.VMEM((steps, tiles, rows, width), jnp.int16),
            pltpu.VMEM((groups, tiles, rows, LANES), jnp.int16),
            pltpu.VMEM((groups, tiles, rows, LANES), jnp.int16),
            pltpu.VMEM((tiles, rows, full), jnp.float32),
            pltpu.VMEM((tiles, rows, full), jnp.float32),
            pltpu.VMEM((tiles, rows, full), jnp.float32),
            pltpu.VMEM((tiles, rows, full), jnp.float32),
            pltpu.VMEM((steps, tiles, 2, width), jnp.float32),
            pltpu.VMEM((steps, tiles, 2, width), jnp.float32),
            pltpu.VMEM((tiles, rows, width), jnp.float32),
            pltpu.VMEM((steps, total_rows, full), jnp.float32),
            pltpu.VMEM((steps, total_rows, full), jnp.float32),
            pltpu.VMEM((steps, LANES), jnp.float32),
            pltpu.VMEM((tiles, steps, LANES), jnp.float32),
            dma((steps,)), dma((steps,)),
            dma((lines, steps)), dma((lines, steps)),
            dma((lines, steps)), dma((lines, steps)),
            dma((lines, steps)), dma((lines, steps)),
            dma((steps,)), dma((steps,)),
            dma((groups,)), dma((groups,)),
            dma((2,)), dma((2,)),
            dma((steps,)), dma((steps,)),
            dma((2,)), dma((2,)), dma((1,)),
        ],
        compiler_params=pltpu.CompilerParams(collective_id=0, has_side_effects=True),
    )(weights, terminal[0], density_history[0], density_init[0])
    values, density = pl.pallas_call(
        finish,
        out_shape=(
            jax.ShapeDtypeStruct((steps, rows, cols), jnp.float32),
            jax.ShapeDtypeStruct((rows, cols), jnp.float32),
        ),
        in_specs=[anywhere, anywhere],
        out_specs=(anywhere, anywhere),
        scratch_shapes=[dma((2,))],
        compiler_params=pltpu.CompilerParams(vmem_limit_bytes=8 * 1024 * 1024),
    )(values, density)
    return values[None], density[None]


def solution(mesh):
    in_specs = (P(), P("pop", "tile", None), P("pop", None, "tile", None), P("pop", "tile", None))
    out_specs = (P("pop", None, "tile", None), P("pop", "tile", None))
    body = functools.partial(per_device, mesh.shape["pop"], mesh.shape["tile"])
    return jax.shard_map(body, mesh=mesh, in_specs=in_specs, out_specs=out_specs, check_vma=False)
```

```python
import functools

import jax
import jax.numpy as jnp
from jax import lax
from jax.experimental import pallas as pl
from jax.experimental.pallas import tpu as pltpu
from jax.sharding import PartitionSpec as P

time_step = 0.2
viscosity = 0.2
LANES = 128
WINDOWS = 4
SPAN = LANES // WINDOWS
CHUNK = 512
BOTH = (0, 1)
CENTRE = 1.1
LARGEST = 3.0 * 0.901
LEVELS = 32400.0
RELAY = (2.6, 0.35)
PARTIAL = (3.6, 0.35)
TOTAL = (6.4, 0.6)
SWEEP = (12.5, 0.9)
STRIP = (20.0, 0.65)


def kernel(pops, tiles, weights_in, terminal_in, history_in, initial_in, values, density_out,
           weights, terminal, history, initial, load_sem, near_other, near, near_relay, own_sum, part_out, part_in,
           cost_out, cost_in, rim_out, rim_in, value_out, start_value, mass_out, start_mass, edge_out, edge_in, mass_main, slope_r, slope_c, sums_own, sums_all,
           other_send, other_recv, near_send, near_recv, relay_send, relay_recv, part_send, part_recv,
           cost_send, cost_recv, rim_send, rim_recv, start_send, start_recv,
           edge_send, edge_recv, back_send, back_recv, back_self):
    steps, rows, cols = history.shape
    width = cols // tiles
    full = width + LANES
    total_rows = tiles * rows
    outer = pops // 4
    me = lax.axis_index("tile")
    own = lax.axis_index("pop")
    core = own % 2
    plane = (own // 2) % 2
    line = own // 4

    def pop_of(a, b, c):
        return (a * 2 + b) * 2 + c

    partner = pop_of(line, plane, 1 - core)
    across = pop_of(line, 1 - plane, core)
    columns = [pop_of((line + j) % outer, plane, core) for j in range(1, outer)]
    behind = [(line + outer - j) % outer for j in range(1, outer)]

    def along_row(n):
        return n % 2 == 0 or outer == 1

    def first_peers(n):
        return [across] if along_row(n) else columns

    def flipped(q):
        return q + 1 - 2 * (q % 2)

    def second_peers(n):
        return columns if along_row(n) else [across]

    def sources(n):
        far = [(line, 1 - plane)] if along_row(n) else [(a, plane) for a in behind]
        return [own, partner] + [pop_of(a, b, core) for a, b in far] + [pop_of(a, b, 1 - core) for a, b in far]

    lower = 1 - me // (tiles // 2)
    peers = [(me + d + lower * (tiles - 2 * d)) % tiles for d in range(1, tiles)]

    barrier = pltpu.get_barrier_semaphore()
    greeted = [{"tile": z} for z in peers] + [{"pop": q} for q in [partner, across] + columns + [flipped(q) for q in [across] + columns]]
    for there in greeted:
        pl.semaphore_signal(barrier, inc=1, device_id=there, device_id_type=pl.DeviceIdType.MESH)

    loads = [pltpu.make_async_copy(src, dst, load_sem.at[n]) for n, (src, dst) in enumerate(
        [(weights_in, weights), (terminal_in, terminal), (initial_in, initial), (history_in, history)])]
    for load in loads:
        load.start()
    for load in loads:
        load.wait()
    lane = lax.broadcasted_iota(jnp.int32, (rows, LANES), 1)
    window = ((lane + SPAN // 2) % LANES) // SPAN
    right_side = lax.broadcasted_iota(jnp.int32, (rows, LANES), 1) < LANES // 2

    def main_of(block, z):
        return block[:, z * width:(z + 1) * width]

    def rim_of(block, z):
        right = ((z + 1) % tiles) * width
        left = ((z + tiles - 1) % tiles) * width + width - LANES
        return jnp.where(right_side, block[:, right:right + LANES], block[:, left:left + LANES])

    for src, dst in [(terminal, value_out), (initial, mass_out)]:
        block = src[...]
        for z in range(tiles):
            dst[z, :, :width] = main_of(block, z)
            dst[z, :, width:] = rim_of(block, z)
    start_value[me] = value_out[me]
    start_mass[me] = mass_out[me]

    pl.semaphore_wait(barrier, len(greeted))

    def cut(z):
        return pl.ds(pl.multiple_of(z * width, LANES), width)

    sent = []

    def remote(src, dst, send, recv, there):
        copy = pltpu.make_async_remote_copy(src_ref=src, dst_ref=dst, send_sem=send, recv_sem=recv,
                                            device_id=there, device_id_type=pl.DeviceIdType.MESH)
        copy.start()
        return copy

    def arrived(ref, sem):
        pltpu.make_async_copy(ref, ref, sem).wait()

    def spread(src, dst, send, recv):
        for z in peers:
            remote(src.at[z], dst.at[me], send, recv, {"tile": z})

    def wait_spread(dst, sem):
        arrived(dst.at[pl.ds(0, tiles - 1)], sem)

    for n in range(steps):
        t = steps - 1 - n
        for j, q in enumerate(first_peers(n)):
            sent.append(remote(history.at[t], near.at[j, t], near_send.at[j, n], near_recv.at[j, n], {"pop": q}))
            if n in BOTH:
                sent.append(remote(history.at[t], near_relay.at[j, t], relay_send.at[j, n], relay_recv.at[j, n],
                                   {"pop": flipped(q)}))
        sent.append(remote(history.at[t], near_other.at[t], other_send.at[n], other_recv.at[n], {"pop": partner}))
    spread(value_out, start_value, start_send.at[0], start_recv.at[0])
    spread(mass_out, start_mass, start_send.at[1], start_recv.at[1])

    def weight(p, q):
        return weights[p, q].astype(jnp.float32) * (1.0 / pops)

    def part_step(n):
        return LARGEST * (4.0 if along_row(n) else 2.0 * outer) / pops / LEVELS

    cost_step = LARGEST / LEVELS

    def coded(x, step):
        return jnp.round(x * (1.0 / step)).astype(jnp.int32).astype(jnp.int16)

    def decoded(x, step):
        return x.astype(jnp.int32).astype(jnp.float32) * step

    def stage_relay(n):
        t = steps - 1 - n
        for j in range(len(first_peers(n))):
            arrived(near.at[j, t], near_recv.at[j, n])
            if n in BOTH:
                continue
            sent.append(remote(near.at[j, t], near_relay.at[j, t], relay_send.at[j, n], relay_recv.at[j, n],
                               {"pop": partner}))

    def stage_partial(n):
        t = steps - 1 - n
        far = range(len(first_peers(n)))
        arrived(near_other.at[t], other_recv.at[n])
        for j in far:
            arrived(near_relay.at[j, t], relay_recv.at[j, n])
        own_factors = [weight(own, q) for q in sources(n)]
        part_factors = [[weight(p, q) for q in sources(n)] for p in second_peers(n)]
        for c in range(0, cols, CHUNK):
            span = slice(c, c + CHUNK)
            blocks = [history[t, :, span], near_other[t, :, span]]
            blocks += [near[j, t, :, span] for j in far] + [near_relay[j, t, :, span] for j in far]
            blocks = [b.astype(jnp.float32) - CENTRE for b in blocks]

            def mixed(factors):
                total = factors[0] * blocks[0]
                for f, b in zip(factors[1:], blocks[1:]):
                    total = total + f * b
                return total

            for j, factors in enumerate(part_factors):
                part_out[j, n, :, span] = coded(mixed(factors), part_step(n))
            own_sum[n, :, span] = mixed(own_factors)
        for j, q in enumerate(second_peers(n)):
            sent.append(remote(part_out.at[j, n], part_in.at[j, n], part_send.at[j, n], part_recv.at[j, n], {"pop": q}))

    def stage_total(n):
        if n == 0:
            wait_spread(start_value, start_recv.at[0])
            send_edges(start_value[:, :, :width].reshape(total_rows, width), 0)
        total = own_sum[n]
        for j in range(len(second_peers(n))):
            arrived(part_in.at[j, n], part_recv.at[j, n])
            total = total + decoded(part_in[j, n], part_step(n))
        own_sum[n] = total
        for z in range(tiles):
            cost_out[n, z] = coded(main_of(total, z), cost_step)
        spread(cost_out.at[n], cost_in.at[n], cost_send.at[n], cost_recv.at[n])
        cost_in[n, me] = cost_out[n, me]
        g, k = n // WINDOWS, n % WINDOWS
        if k == WINDOWS - 1:
            for z in range(tiles):
                rim = rim_of(own_sum[g * WINDOWS], z)
                for i in range(1, WINDOWS):
                    rim = jnp.where(window == i, pltpu.roll(rim_of(own_sum[g * WINDOWS + i], z), SPAN * i, 1), rim)
                rim_out[g, z] = coded(rim, cost_step)
            spread(rim_out.at[g], rim_in.at[g], rim_send.at[g], rim_recv.at[g])
            rim_in[g, me] = rim_out[g, me]

    def ahead_r(x):
        return pltpu.roll(x, total_rows - 1, 0)

    def behind_r(x):
        return pltpu.roll(x, 1, 0)

    def ahead_c(x):
        return pltpu.roll(x, full - 1, 1)

    def behind_c(x):
        return pltpu.roll(x, 1, 1)

    def send_edges(main, n):
        for z in range(tiles):
            above = (z * rows + total_rows - 1) % total_rows
            below = (z * rows + rows) % total_rows
            edge_out[n, z, 0:1, :] = main[above:above + 1, :]
            edge_out[n, z, 1:2, :] = main[below:below + 1, :]
        spread(edge_out.at[n], edge_in.at[n], edge_send.at[n], edge_recv.at[n])
        edge_in[n, me] = edge_out[n, me]

    def send_back(src, dst, n):
        pltpu.make_async_copy(src.at[me], dst.at[:, cut(me)], back_self.at[n]).start()
        for z in peers:
            remote(src.at[z], dst.at[:, cut(me)], back_send.at[n], back_recv.at[n], {"tile": z})

    def wait_back(src, dst, n):
        pltpu.make_async_copy(src.at[me], dst.at[:, cut(me)], back_self.at[n]).wait()
        landed = dst.at[:, pl.ds(0, (tiles - 1) * width)]
        arrived(landed, back_recv.at[n])
        arrived(landed, back_send.at[n])

    state = {}

    def stage_sweep(n):
        t = steps - 1 - n
        if n == 0:
            state["u"] = start_value[...].reshape(total_rows, full)
        wait_spread(cost_in.at[n], cost_recv.at[n])
        g, k = n // WINDOWS, n % WINDOWS
        if k == 0:
            wait_spread(rim_in.at[g], rim_recv.at[g])
            state["rim"] = decoded(rim_in[g], cost_step).reshape(total_rows, LANES)
        rim = state["rim"] if k == 0 else pltpu.roll(state["rim"], LANES - SPAN * k, 1)
        source = jnp.concatenate([decoded(cost_in[n], cost_step).reshape(total_rows, width), rim], axis=1)
        u = state["u"]
        dr = ahead_r(u) - u
        dc = ahead_c(u) - u
        if t + 1 < steps:
            slope_r[t + 1] = dr
            slope_c[t + 1] = dc
        er, ec = behind_r(dr), behind_c(dc)
        br, bc = jnp.maximum(er, 0.0), jnp.maximum(ec, 0.0)
        ar, ac = jnp.minimum(dr, 0.0), jnp.minimum(dc, 0.0)
        lap = (dr - er) + (dc - ec)
        ham = 0.5 * ((br * br + ar * ar) + (bc * bc + ac * ac))
        u = u + time_step * (viscosity * lap - ham + source)
        state["u"] = u
        main = u[:, :width]
        if t > 0:
            send_edges(main, n + 1)
        line_sum = jnp.sum(main, axis=0, keepdims=True)
        folded = line_sum[:, :LANES]
        for j in range(1, width // LANES):
            folded = folded + line_sum[:, j * LANES:(j + 1) * LANES]
        sums_own[t:t + 1, :] = folded

    row = lax.broadcasted_iota(jnp.int32, (rows, cols), 0)

    def stage_strip(n):
        t = steps - 1 - n
        wait_spread(edge_in.at[n], edge_recv.at[n])
        above = jnp.concatenate([edge_in[n, z, 0:1, :] for z in range(tiles)], axis=1)
        below = jnp.concatenate([edge_in[n, z, 1:2, :] for z in range(tiles)], axis=1)
        u = terminal[...] if n == 0 else values[t + 1]
        dr = jnp.where(row == rows - 1, below, pltpu.roll(u, rows - 1, 0)) - u
        er = u - jnp.where(row == 0, above, pltpu.roll(u, 1, 0))
        dc = pltpu.roll(u, cols - 1, 1) - u
        ec = pltpu.roll(dc, 1, 1)
        br, bc = jnp.maximum(er, 0.0), jnp.maximum(ec, 0.0)
        ar, ac = jnp.minimum(dr, 0.0), jnp.minimum(dc, 0.0)
        lap = (dr - er) + (dc - ec)
        ham = 0.5 * ((br * br + ar * ar) + (bc * bc + ac * ac))
        values[t] = u + time_step * (viscosity * lap - ham + own_sum[n])

    stages = [(RELAY, stage_relay), (PARTIAL, stage_partial), (TOTAL, stage_total), (SWEEP, stage_sweep), (STRIP, stage_strip)]
    plan = sorted((first + per * n, k, n) for k, ((first, per), _) in enumerate(stages) for n in range(steps))
    last = plan.index((SWEEP[0] + SWEEP[1] * (steps - 1), 3, steps - 1)) + 1
    for _, k, n in plan[:last]:
        stages[k][1](n)

    sums_n = 1
    sums_all[me] = sums_own[...]
    for z in peers:
        remote(sums_own, sums_all.at[me], back_send.at[sums_n], back_recv.at[sums_n], {"tile": z})

    wait_spread(start_mass, start_recv.at[1])
    u = state["u"]
    mass = start_mass[...].reshape(total_rows, full)
    for t in range(steps):
        if t == 0:
            dr, dc = ahead_r(u) - u, ahead_c(u) - u
        else:
            dr, dc = slope_r[t], slope_c[t]
        pr, qr = viscosity + jnp.maximum(dr, 0.0), viscosity + jnp.maximum(-dr, 0.0)
        pc, qc = viscosity + jnp.maximum(dc, 0.0), viscosity + jnp.maximum(-dc, 0.0)
        ec = behind_c(dc)
        bc, kc = viscosity + jnp.maximum(ec, 0.0), viscosity + jnp.maximum(-ec, 0.0)
        net_r = pr * ahead_r(mass) - qr * mass
        net_c = (pc * ahead_c(mass) - qc * mass) - (bc * mass - kc * behind_c(mass))
        mass = mass + time_step * ((net_r - behind_r(net_r)) + net_c)
    mass_main[...] = mass[:, :width].reshape(tiles, rows, width)
    send_back(mass_main, density_out, 0)
    wait_spread(start_value, start_send.at[0])
    wait_spread(start_mass, start_send.at[1])
    for g in range(steps // WINDOWS):
        wait_spread(rim_in.at[g], rim_send.at[g])
    for n in range(steps):
        wait_spread(cost_in.at[n], cost_send.at[n])
    for copy in sent:
        copy.wait_send()
    for _, k, n in plan[last:]:
        stages[k][1](n)

    arrived(sums_all.at[pl.ds(0, tiles - 1)], back_recv.at[sums_n])
    arrived(sums_all.at[pl.ds(0, tiles - 1)], back_send.at[sums_n])
    grand = jnp.sum(jnp.sum(sums_all[...], axis=0), axis=1, keepdims=True) * (1.0 / (total_rows * cols))
    for t in reversed(range(steps)):
        values[t] = values[t] - grand[t:t + 1, :]
    wait_back(mass_main, density_out, 0)
    for n in range(steps):
        wait_spread(edge_in.at[n], edge_send.at[n])


def finish(values, density, values_out, density_out, sems):
    copies = [
        pltpu.make_async_copy(values, values_out, sems.at[0]),
        pltpu.make_async_copy(density, density_out, sems.at[1]),
    ]
    for copy in copies:
        copy.start()
    for copy in copies:
        copy.wait()


def per_device(pops, tiles, weights, terminal, density_history, density_init):
    _, steps, rows, cols = density_history.shape
    width = cols // tiles
    outer = pops // 4
    total_rows = tiles * rows
    full = width + LANES
    dma = pltpu.SemaphoreType.DMA
    lines = max(outer - 1, 1)
    groups = steps // WINDOWS
    vmem = pl.BlockSpec(memory_space=pltpu.VMEM)
    anywhere = pl.BlockSpec(memory_space=pl.ANY)
    values, density = pl.pallas_call(
        functools.partial(kernel, pops, tiles),
        out_shape=(
            pltpu.VMEM((steps, rows, cols), jnp.float32),
            pltpu.VMEM((rows, cols), jnp.float32),
        ),
        in_specs=[anywhere, anywhere, anywhere, anywhere],
        out_specs=(vmem, vmem),
        scratch_shapes=[
            pltpu.SMEM((pops, pops), jnp.int32),
            pltpu.VMEM((rows, cols), jnp.float32),
            pltpu.VMEM((steps, rows, cols), jnp.bfloat16),
            pltpu.VMEM((rows, cols), jnp.float32),
            dma((4,)),
            pltpu.VMEM((steps, rows, cols), jnp.bfloat16),
            pltpu.VMEM((lines, steps, rows, cols), jnp.bfloat16),
            pltpu.VMEM((lines, steps, rows, cols), jnp.bfloat16),
            pltpu.VMEM((steps, rows, cols), jnp.float32),
            pltpu.VMEM((lines, steps, rows, cols), jnp.int16),
            pltpu.VMEM((lines, steps, rows, cols), jnp.int16),
            pltpu.VMEM((steps, tiles, rows, width), jnp.int16),
            pltpu.VMEM((steps, tiles, rows, width), jnp.int16),
            pltpu.VMEM((groups, tiles, rows, LANES), jnp.int16),
            pltpu.VMEM((groups, tiles, rows, LANES), jnp.int16),
            pltpu.VMEM((tiles, rows, full), jnp.float32),
            pltpu.VMEM((tiles, rows, full), jnp.float32),
            pltpu.VMEM((tiles, rows, full), jnp.float32),
            pltpu.VMEM((tiles, rows, full), jnp.float32),
            pltpu.VMEM((steps, tiles, 2, width), jnp.float32),
            pltpu.VMEM((steps, tiles, 2, width), jnp.float32),
            pltpu.VMEM((tiles, rows, width), jnp.float32),
            pltpu.VMEM((steps, total_rows, full), jnp.float32),
            pltpu.VMEM((steps, total_rows, full), jnp.float32),
            pltpu.VMEM((steps, LANES), jnp.float32),
            pltpu.VMEM((tiles, steps, LANES), jnp.float32),
            dma((steps,)), dma((steps,)),
            dma((lines, steps)), dma((lines, steps)),
            dma((lines, steps)), dma((lines, steps)),
            dma((lines, steps)), dma((lines, steps)),
            dma((steps,)), dma((steps,)),
            dma((groups,)), dma((groups,)),
            dma((2,)), dma((2,)),
            dma((steps,)), dma((steps,)),
            dma((2,)), dma((2,)), dma((1,)),
        ],
        compiler_params=pltpu.CompilerParams(collective_id=0, has_side_effects=True),
    )(weights, terminal[0], density_history[0], density_init[0])
    values, density = pl.pallas_call(
        finish,
        out_shape=(
            jax.ShapeDtypeStruct((steps, rows, cols), jnp.float32),
            jax.ShapeDtypeStruct((rows, cols), jnp.float32),
        ),
        in_specs=[anywhere, anywhere],
        out_specs=(anywhere, anywhere),
        scratch_shapes=[dma((2,))],
        compiler_params=pltpu.CompilerParams(vmem_limit_bytes=8 * 1024 * 1024),
    )(values, density)
    return values[None], density[None]


def solution(mesh):
    in_specs = (P(), P("pop", "tile", None), P("pop", None, "tile", None), P("pop", "tile", None))
    out_specs = (P("pop", None, "tile", None), P("pop", "tile", None))
    body = functools.partial(per_device, mesh.shape["pop"], mesh.shape["tile"])
    return jax.shard_map(body, mesh=mesh, in_specs=in_specs, out_specs=out_specs, check_vma=False)
```
